32 devices in a mesh: shard: 8 (over z, x), width: 4 (over y, core).
Axes of the slice: x: 2, y: 2, z: 4, core: 2. Of those that a mesh axis runs over, the one named last changes fastest.
Arguments:
- w_query: float32 [4096, 4096], P('shard', 'width'), may hold values from -0.125 to 0.125
- first_query: float32 [4096, 4096], P('shard', 'width'), may hold values from -0.09375 to 0.09375
- second_query: float32 [4096, 4096], P('shard', 'width'), may hold values from -0.09375 to 0.09375
- w_key: float32 [4096, 1024], P('shard', 'width'), may hold values from -0.125 to 0.125
- first_key: float32 [4096, 1024], P('shard', 'width'), may hold values from -0.09375 to 0.09375
- second_key: float32 [4096, 1024], P('shard', 'width'), may hold values from -0.09375 to 0.09375
- w_value: float32 [4096, 1024], P('shard', 'width'), may hold values from -0.125 to 0.125
- first_value: float32 [4096, 1024], P('shard', 'width'), may hold values from -0.09375 to 0.09375
- second_value: float32 [4096, 1024], P('shard', 'width'), may hold values from -0.09375 to 0.09375
- norm_train: float32 [4096], P(('shard', 'width')), may hold values from 0.25 to 1.75
- norm_step: float32 [4096], P(('shard', 'width')), may hold values from -0.3 to 0.3
Outputs:
- serving_query: bfloat16 [4096, 4096], P(None, 'width')
- serving_key: bfloat16 [4096, 1024], P(None, 'width')
- serving_value: bfloat16 [4096, 1024], P(None, 'width')
- column_query: float32 [4096], P('width')
- column_key: float32 [1024], P('width')
- column_value: float32 [1024], P('width')
- serve_norm: bfloat16 [4096], replicated
- whole_query: float32 [4096, 4096], P('shard', 'width')
- whole_key: float32 [4096, 1024], P('shard', 'width')
- whole_value: float32 [4096, 1024], P('shard', 'width')
The draws below stay inside these ranges and needn't reach their ends.
All inputs are finite; a program needn't handle non-finite values. Where the reference program divides by a largest or mean magnitude, that divisor is 1e-20 or more.
Results may differ from the reference program's by a relative error of at most 0.0004.
Values may be sent and summed in bfloat16 or wider, within the bound.
A program may use at most 128 MiB of HBM per device.

```python
import jax
import jax.numpy as jnp

D_MODEL = 4096
Q_DIM = 4096
KV_DIM = 1024


def raised(entries, stream_key, source, target, parts, factor):
    owner, partner = [(jnp.arange(entries.shape[dim]) // (entries.shape[dim] // parts)).reshape([-1 if axis == dim else 1 for axis in range(entries.ndim)]) for dim in (source, target)]
    chosen = jax.random.permutation(stream_key, parts)[partner]
    strong = (owner == chosen) | (owner == (partner + parts // 2) % parts)
    return jnp.where(strong, factor * entries, entries)


def block_levels(own_key, shape, pieces, least, high):
    loudness = 1.0
    for dim, parts in pieces:
        steps = jax.random.uniform(jax.random.fold_in(jax.random.fold_in(own_key, 6), dim), (parts,), jnp.float32, least / len(pieces), high / len(pieces))
        loudness = loudness * jnp.repeat(jnp.exp(steps), shape[dim] // parts).reshape((-1,) + (1,) * (len(shape) - 1 - dim))
    return loudness


def scatter_about(key, extent, spread, most, split=(), held_as=jnp.bfloat16):
    array = spread * jax.random.normal(key, extent, jnp.float32)
    if split:
        array = array * block_levels(key, extent, split, -0.22, 0.18)
    return jnp.clip(array, -most, most).astype(held_as)


def gaussian_with(stream_key, dims, deviation, reach, split, heavy, held_as=jnp.bfloat16):
    values = deviation * jax.random.normal(stream_key, dims, jnp.float32)
    if split:
        values = values * block_levels(stream_key, dims, split, -0.22, 0.18)
    return jnp.clip(raised(values, jax.random.fold_in(stream_key, 3), *heavy), -reach, reach).astype(held_as)


def setup_inputs(seed: int = 0) -> dict:
    seeds = jax.random.split(jax.random.key(seed), 12)
    return {
        "w_query": gaussian_with(seeds[0], (D_MODEL, Q_DIM), D_MODEL ** -0.5, 0.125, ((0, 8), (1, 4)), (0, 1, 8, 2.0), jnp.float32),
        "first_query": scatter_about(seeds[1], (D_MODEL, Q_DIM), D_MODEL ** -0.5, 0.09375, ((0, 8), (1, 4)), jnp.float32),
        "second_query": scatter_about(seeds[2], (D_MODEL, Q_DIM), D_MODEL ** -0.5, 0.09375, ((0, 8), (1, 4)), jnp.float32),
        "w_key": gaussian_with(seeds[3], (D_MODEL, KV_DIM), D_MODEL ** -0.5, 0.125, ((0, 8), (1, 4)), (0, 1, 8, 2.0), jnp.float32),
        "first_key": scatter_about(seeds[4], (D_MODEL, KV_DIM), D_MODEL ** -0.5, 0.09375, ((0, 8), (1, 4)), jnp.float32),
        "second_key": scatter_about(seeds[5], (D_MODEL, KV_DIM), D_MODEL ** -0.5, 0.09375, ((0, 8), (1, 4)), jnp.float32),
        "w_value": gaussian_with(seeds[6], (D_MODEL, KV_DIM), D_MODEL ** -0.5, 0.125, ((0, 8), (1, 4)), (0, 1, 8, 2.0), jnp.float32),
        "first_value": scatter_about(seeds[7], (D_MODEL, KV_DIM), D_MODEL ** -0.5, 0.09375, ((0, 8), (1, 4)), jnp.float32),
        "second_value": scatter_about(seeds[8], (D_MODEL, KV_DIM), D_MODEL ** -0.5, 0.09375, ((0, 8), (1, 4)), jnp.float32),
        "norm_train": jnp.clip(1.0 + 0.15 * jax.random.normal(seeds[9], (D_MODEL,), jnp.float32), 0.25, 1.75),
        "norm_step": jnp.clip(jax.random.uniform(seeds[10], (D_MODEL,), jnp.float32, -0.3, 0.3) * block_levels(seeds[10], (D_MODEL,), ((0, 32),), -0.4, 0.0), -0.3, 0.3),
    }


learn_rate = 0.2
hold_rate = 0.8


def reference(w_query, first_query, second_query, w_key, first_key, second_key, w_value, first_value, second_value, norm_train, norm_step):
    hold_query = hold_rate * first_query + second_query
    whole_query = w_query - learn_rate * hold_query
    hold_key = hold_rate * first_key + second_key
    whole_key = w_key - learn_rate * hold_key
    hold_value = hold_rate * first_value + second_value
    whole_value = w_value - learn_rate * hold_value
    column_query = jnp.sum(jnp.abs(whole_query), axis=0) / D_MODEL
    serving_query = (whole_query / column_query).astype(jnp.bfloat16)
    column_key = jnp.sum(jnp.abs(whole_key), axis=0) / D_MODEL
    serving_key = (whole_key / column_key).astype(jnp.bfloat16)
    column_value = jnp.sum(jnp.abs(whole_value), axis=0) / D_MODEL
    serving_value = (whole_value / column_value).astype(jnp.bfloat16)
    serve_norm = (norm_train + norm_step).astype(jnp.bfloat16)
    return serving_query, serving_key, serving_value, column_query, column_key, column_value, serve_norm, whole_query, whole_key, whole_value
```

```python
import functools

import jax
import jax.numpy as jnp
from jax import lax
from jax.experimental import pallas as pl
from jax.experimental.pallas import tpu as pltpu
from jax.sharding import PartitionSpec as P

learn_rate = 0.2
hold_rate = 0.8
MESH = pl.DeviceIdType.MESH
TILE = 16
DOWN, UP, CROSS = 0, 1, 2


def plan_units(rows, extents):
    least = min(extents)
    units = []
    for i in sorted(range(len(extents)), key=lambda i: extents[i]):
        count = max(1, min(extents[i] // least, rows // TILE))
        size = rows // count
        units += [(i, j * size, size) for j in range(count)]
    return units


def gather_kernel(
    n,
    width,
    units,
    w_q,
    first_q,
    second_q,
    w_k,
    first_k,
    second_k,
    w_v,
    first_v,
    second_v,
    norm_train,
    norm_step,
    out_q,
    out_k,
    out_v,
    whole_q,
    whole_k,
    whole_v,
    col_q,
    col_k,
    col_v,
    norm_out,
    in_q,
    in_k,
    in_v,
    sums_q,
    sums_k,
    sums_v,
    in_norm,
    norm_sem,
    load_sem,
    sum_send,
    sum_recv,
    wid_send,
    wid_recv,
    nrm_send,
    nrm_recv,
    link_send,
    link_recv,
):
    me = lax.axis_index("shard")
    me_w = lax.axis_index("width")
    depth = n // 2
    z, x = lax.div(me, 2), lax.rem(me, 2)
    count = len(units)
    half = count // 2
    outs, wholes, cols = (out_q, out_k, out_v), (whole_q, whole_k, whole_v), (col_q, col_k, col_v)
    stages, sums = (in_q, in_k, in_v), (sums_q, sums_k, sums_v)
    sources = ((w_q, first_q, second_q), (w_k, first_k, second_k), (w_v, first_v, second_v))
    rows = whole_q.shape[0]
    order = list(dict.fromkeys(unit[0] for unit in units))

    barrier = pltpu.get_barrier_semaphore()
    for k in range(1, n):
        pl.semaphore_signal(
            barrier, inc=1, device_id={"shard": lax.rem(me + k, n)}, device_id_type=MESH
        )
    for k in range(1, width):
        pl.semaphore_signal(
            barrier, inc=1, device_id={"width": lax.rem(me_w + k, width)}, device_id_type=MESH
        )

    loads = []
    for u, (i, at, size) in enumerate(units):
        group = []
        for j in range(3):
            copy = pltpu.make_async_copy(
                sources[i][j].at[pl.ds(at, size)], stages[i].at[j, pl.ds(at, size)], load_sem.at[u, j]
            )
            copy.start()
            group.append(copy)
        loads.append(group)
    norm_loads = [
        pltpu.make_async_copy(ref, in_norm.at[j], norm_sem.at[j])
        for j, ref in enumerate((norm_train, norm_step))
    ]
    for copy in norm_loads:
        copy.start()

    sum_copies = {}
    wid_copies = []
    met = False
    for i in order:
        stage, whole = stages[i], wholes[i]
        total = jnp.zeros((8, whole.shape[1]), jnp.float32)
        for u, (owner, at, size) in enumerate(units):
            if owner != i:
                continue
            for copy in loads[u]:
                copy.wait()

            def update(r, total, at=at, stage=stage, whole=whole):
                for j in range(TILE // 8):
                    here = pl.ds(pl.multiple_of(at + r * TILE + j * 8, 8), 8)
                    new = stage[0, here] - learn_rate * (hold_rate * stage[1, here] + stage[2, here])
                    whole[here, :] = new
                    total = total + jnp.abs(new)
                return total

            total = lax.fori_loop(0, size // TILE, update, total)
        sums[i][me] = jnp.sum(total, axis=0, keepdims=True)
        if not met:
            for copy in norm_loads:
                copy.wait()
            norm_out[me, me_w] = in_norm[0] + in_norm[1]
            pl.semaphore_wait(barrier, n - 1 + width - 1)
        sum_copies[i] = []
        for k in range(1, n):
            copy = pltpu.make_async_remote_copy(
                src_ref=sums[i].at[me],
                dst_ref=sums[i].at[me],
                send_sem=sum_send.at[i, k - 1],
                recv_sem=sum_recv.at[i, k - 1],
                device_id={"shard": lax.rem(me + k, n)},
                device_id_type=MESH,
            )
            copy.start()
            sum_copies[i].append(copy)
        if not met:
            for k in range(1, width):
                copy = pltpu.make_async_remote_copy(
                    src_ref=norm_out.at[me, me_w],
                    dst_ref=norm_out.at[me, me_w],
                    send_sem=wid_send.at[k - 1],
                    recv_sem=wid_recv.at[k - 1],
                    device_id={"width": lax.rem(me_w + k, width)},
                    device_id_type=MESH,
                )
                copy.start()
                wid_copies.append(copy)
        met = True

    targets = (lax.max(z - 1, 0) * 2 + x, lax.min(z + 1, depth - 1) * 2 + x, z * 2 + 1 - x)

    def piece(owner, u, way, slot):
        i, at, size = units[u]
        where = pl.ds(pl.multiple_of(owner * rows + at, TILE), size)
        return pltpu.make_async_remote_copy(
            src_ref=outs[i].at[where],
            dst_ref=outs[i].at[where],
            send_sem=link_send.at[way, slot, u],
            recv_sem=link_recv.at[way, slot, u],
            device_id={"shard": targets[way]},
            device_id_type=MESH,
        )

    def crosses(source, u):
        low = (z >= 1) & (z < depth // 2) & (source == z - 1)
        high = (z >= depth // 2) & (z <= depth - 2) & (source == z + 1)
        no = low | high
        if u >= half:
            no = no | ((z == 0) & (source == depth - 1)) | ((z == depth - 1) & (source == 0))
        return jnp.logical_not(no)

    def send(owner_z, column, u, way, slot):
        piece(owner_z * 2 + column, u, way, slot).start()

    for i in order:
        for copy in sum_copies[i]:
            copy.wait_recv()
        total = sums[i][0]
        for k in range(1, n):
            total = total + sums[i][k]
        col = total / (rows * n)
        cols[i][...] = col
        factor = jnp.broadcast_to(1.0 / col, (TILE, col.shape[1]))
        whole, out = wholes[i], outs[i]
        for u, (owner, at, size) in enumerate(units):
            if owner != i:
                continue

            def narrow(r, carry, at=at, whole=whole, out=out, factor=factor):
                here = pl.multiple_of(at + r * TILE, TILE)
                there = pl.multiple_of(me * rows + at + r * TILE, TILE)
                out[pl.ds(there, TILE), :] = (whole[pl.ds(here, TILE), :] * factor).astype(jnp.bfloat16)
                return carry

            lax.fori_loop(0, size // TILE, narrow, 0)

            @pl.when(z >= 1)
            def _(u=u):
                send(z, x, u, DOWN, 0)

            @pl.when(z <= depth - 2)
            def _(u=u):
                send(z, x, u, UP, 0)

            send(z, x, u, CROSS, 0)

    for copy in wid_copies:
        copy.wait_recv()
    nrm_copies = []
    for k in range(1, n):
        copy = pltpu.make_async_remote_copy(
            src_ref=norm_out.at[me],
            dst_ref=norm_out.at[me],
            send_sem=nrm_send.at[k - 1],
            recv_sem=nrm_recv.at[k - 1],
            device_id={"shard": lax.rem(me + k, n)},
            device_id_type=MESH,
        )
        copy.start()
        nrm_copies.append(copy)

    last = depth - 1
    low_end, high_end = z <= depth // 2 - 2, z >= depth // 2 + 1

    def step(t, carry):
        for u in range(count):

            @pl.when(z + t <= last)
            def _(u=u):
                piece(me, u, DOWN, t - 1).wait_recv()

                @pl.when(z >= 1)
                def _():
                    send(z + t, x, u, DOWN, t)

                @pl.when(crosses(z + t, u))
                def _():
                    send(z + t, x, u, CROSS, t)

            @pl.when(z - t >= 0)
            def _(u=u):
                piece(me, u, UP, t - 1).wait_recv()

                @pl.when(z <= depth - 2)
                def _():
                    send(z - t, x, u, UP, t)

                @pl.when(crosses(z - t, u))
                def _():
                    send(z - t, x, u, CROSS, depth - t)

            @pl.when((t == 1) & (low_end | high_end))
            def _(u=u):
                piece(me, u, CROSS, 0).wait_recv()

                @pl.when(low_end)
                def _():
                    send(z, 1 - x, u, UP, last)

                @pl.when(high_end)
                def _():
                    send(z, 1 - x, u, DOWN, last)

            if u >= half:

                @pl.when((t == last) & (z == 1))
                def _(u=u):
                    piece(me, u, CROSS, depth - 2).wait_recv()
                    send(last, 1 - x, u, DOWN, last)

                @pl.when((t == last) & (z == depth - 2))
                def _(u=u):
                    piece(me, u, CROSS, 2).wait_recv()
                    send(0, 1 - x, u, UP, last)

        return carry

    lax.fori_loop(1, depth, step, 0)

    for u in range(count):
        seen = low_end | high_end

        @pl.when(jnp.logical_not(seen))
        def _(u=u):
            piece(me, u, CROSS, 0).wait_recv()

    def remaining(t, carry):
        source = lax.rem(z + t, depth)
        for u in range(count):
            owed = crosses(source, u)
            if u >= half:
                seen = ((z == 1) & (source == last)) | ((z == depth - 2) & (source == 0))
                owed = owed & jnp.logical_not(seen)

            @pl.when(owed)
            def _(u=u):
                piece(me, u, CROSS, t).wait_recv()

        return carry

    lax.fori_loop(1, depth, remaining, 0)
    for u in range(count):
        from_above = (z >= depth // 2) & (z <= depth - 2)
        from_below = (z >= 1) & (z < depth // 2)
        if u >= half:
            from_above = from_above | (z == 0)
            from_below = from_below | (z == last)

        @pl.when(from_above)
        def _(u=u):
            piece(me, u, DOWN, last).wait_recv()

        @pl.when(from_below)
        def _(u=u):
            piece(me, u, UP, last).wait_recv()

    for copy in nrm_copies:
        copy.wait_recv()
    for i in order:
        for copy in sum_copies[i]:
            copy.wait_send()
    for copy in wid_copies + nrm_copies:
        copy.wait_send()

    def sent(t, carry):
        source = lax.rem(z + t, depth)
        for u in range(count):

            @pl.when((z >= 1) & (z + t <= last))
            def _(u=u):
                piece(me, u, DOWN, t).wait_send()

            @pl.when((z <= depth - 2) & (z - t >= 0))
            def _(u=u):
                piece(me, u, UP, t).wait_send()

            @pl.when(crosses(source, u))
            def _(u=u):
                piece(me, u, CROSS, t).wait_send()

        return carry

    lax.fori_loop(0, depth, sent, 0)
    for u in range(count):
        to_above, to_below = low_end, high_end
        if u >= half:
            to_above = to_above | (z == depth - 2)
            to_below = to_below | (z == 1)

        @pl.when(to_above)
        def _(u=u):
            piece(me, u, UP, last).wait_send()

        @pl.when(to_below)
        def _(u=u):
            piece(me, u, DOWN, last).wait_send()


def write_kernel(parts, *refs):
    size = len(refs) - 2
    moved = size // 2
    ins, norm_in, results, norm_out, sems = refs[:moved], refs[moved], refs[moved + 1 : -2], refs[-2], refs[-1]
    copies = []
    for i, (ref, result) in enumerate(zip(ins, results)):
        pieces = parts[i]
        rows = ref.shape[0] // pieces
        for j in range(pieces):
            where = pl.ds(j * rows, rows)
            copy = pltpu.make_async_copy(ref.at[where], result.at[where], sems.at[len(copies)])
            copy.start()
            copies.append(copy)
    norm_out[...] = norm_in[...].astype(jnp.bfloat16)
    for copy in copies:
        copy.wait()


def local(
    n,
    width,
    w_query,
    first_query,
    second_query,
    w_key,
    first_key,
    second_key,
    w_value,
    first_value,
    second_value,
    norm_train,
    norm_step,
):
    groups = ((w_query, first_query, second_query), (w_key, first_key, second_key), (w_value, first_value, second_value))
    rows = w_query.shape[0]
    extents = [each[0].shape[1] for each in groups]
    units = plan_units(rows, extents)
    piece = norm_train.shape[0]
    depth = n // 2
    dma = pltpu.SemaphoreType.DMA
    vmem = pl.BlockSpec(memory_space=pltpu.VMEM)
    hbm = pl.BlockSpec(memory_space=pltpu.HBM)
    shapes = [jax.ShapeDtypeStruct((rows * n, e), jnp.bfloat16) for e in extents]
    shapes += [jax.ShapeDtypeStruct((rows, e), jnp.float32) for e in extents]
    shapes += [jax.ShapeDtypeStruct((1, e), jnp.float32) for e in extents]
    gathered = pl.pallas_call(
        functools.partial(gather_kernel, n, width, units),
        out_shape=shapes + [jax.ShapeDtypeStruct((n, width, 1, piece), jnp.float32)],
        in_specs=[hbm] * 11,
        out_specs=[vmem] * 10,
        scratch_shapes=[pltpu.VMEM((3, rows, e), jnp.float32) for e in extents]
        + [pltpu.VMEM((n, 1, e), jnp.float32) for e in extents]
        + [
            pltpu.VMEM((2, 1, piece), jnp.float32),
            dma((2,)),
            dma((len(units), 3)),
            dma((3, n - 1)),
            dma((3, n - 1)),
            dma((width - 1,)),
            dma((width - 1,)),
            dma((n - 1,)),
            dma((n - 1,)),
            dma((3, depth, len(units))),
            dma((3, depth, len(units))),
        ],
        compiler_params=pltpu.CompilerParams(
            collective_id=0, has_side_effects=True, vmem_limit_bytes=16 * 1024 * 1024
        ),
    )(
        *[pltpu.with_memory_space_constraint(each, pltpu.HBM) for group in groups for each in group],
        pltpu.with_memory_space_constraint(norm_train.reshape(1, -1), pltpu.HBM),
        pltpu.with_memory_space_constraint(norm_step.reshape(1, -1), pltpu.HBM),
    )
    moved, gain = gathered[:-1], gathered[-1].reshape(-1, 128)
    parts = [max(1, each.size * each.dtype.itemsize // (1 << 20)) for each in moved]
    written = pl.pallas_call(
        functools.partial(write_kernel, parts),
        out_shape=shapes + [jax.ShapeDtypeStruct(gain.shape, jnp.bfloat16)],
        in_specs=[vmem] * 10,
        out_specs=[hbm] * 9 + [vmem],
        scratch_shapes=[dma((sum(parts),))],
        compiler_params=pltpu.CompilerParams(vmem_limit_bytes=16 * 1024 * 1024),
    )(*moved, gain)
    serving, whole, column = written[:3], written[3:6], written[6:9]
    return (*serving, *[each.reshape(-1) for each in column], written[9].reshape(-1), *whole)


def solution(mesh):
    split = P("shard", "width")
    both = P(("shard", "width"))
    n, width = mesh.shape["shard"], mesh.shape["width"]
    return jax.shard_map(
        functools.partial(local, n, width),
        mesh=mesh,
        in_specs=(split,) * 9 + (both, both),
        out_specs=(P(None, "width"),) * 3 + (P("width"),) * 3 + (P(),) + (split,) * 3,
        check_vma=False,
    )
```

```python
import functools
import math

import jax
import jax.numpy as jnp
from jax import lax
from jax.experimental import pallas as pl
from jax.experimental.pallas import tpu as pltpu
from jax.sharding import PartitionSpec as P

learn_rate = 0.2
hold_rate = 0.8
MESH = pl.DeviceIdType.MESH
TILE = 16
DOWN, UP, CROSS = 0, 1, 2


def plan_units(rows, extents):
    least = min(extents)
    units = []
    for i in sorted(range(len(extents)), key=lambda i: extents[i]):
        count = max(1, min(extents[i] // least, rows // TILE))
        if not units:
            count = max(2, count)
        size = rows // count
        units += [(i, j * size, size) for j in range(count)]
    return units


def half_of(units, extents):
    sizes = [extents[i] * size for i, _, size in units]
    return min(range(1, len(units)), key=lambda u: abs(2 * sum(sizes[:u]) - sum(sizes)))


def loop_rows(size, extent):
    return math.gcd(size, max(TILE, 16 * 1024 // extent))


def gather_kernel(
    n,
    width,
    units,
    w_q,
    first_q,
    second_q,
    w_k,
    first_k,
    second_k,
    w_v,
    first_v,
    second_v,
    norm_train,
    norm_step,
    out_q,
    out_k,
    out_v,
    whole_q,
    whole_k,
    whole_v,
    col_q,
    col_k,
    col_v,
    norm_out,
    in_q,
    in_k,
    in_v,
    sums_q,
    sums_k,
    sums_v,
    in_norm,
    norm_sem,
    in_early,
    early_send,
    early_recv,
    load_sem,
    sum_send,
    sum_recv,
    wid_send,
    wid_recv,
    nrm_send,
    nrm_recv,
    link_send,
    link_recv,
):
    me = lax.axis_index("shard")
    me_w = lax.axis_index("width")
    depth = n // 2
    z, x = lax.div(me, 2), lax.rem(me, 2)
    count = len(units)
    outs, wholes, cols = (out_q, out_k, out_v), (whole_q, whole_k, whole_v), (col_q, col_k, col_v)
    stages, sums = (in_q, in_k, in_v), (sums_q, sums_k, sums_v)
    sources = ((w_q, first_q, second_q), (w_k, first_k, second_k), (w_v, first_v, second_v))
    rows = whole_q.shape[0]
    half = half_of(units, [each.shape[1] for each in wholes])
    order = list(dict.fromkeys(unit[0] for unit in units))

    barrier = pltpu.get_barrier_semaphore()
    for k in range(1, n):
        pl.semaphore_signal(
            barrier, inc=1, device_id={"shard": lax.rem(me + k, n)}, device_id_type=MESH
        )
    for k in range(1, width):
        pl.semaphore_signal(
            barrier, inc=1, device_id={"width": lax.rem(me_w + k, width)}, device_id_type=MESH
        )

    loads = []
    for u, (i, at, size) in enumerate(units):
        group = []
        for j in range(3):
            copy = pltpu.make_async_copy(
                sources[i][j].at[pl.ds(at, size)], stages[i].at[j, pl.ds(at, size)], load_sem.at[u, j]
            )
            group.append(copy)
        loads.append(group)

    def load(array_is_first):
        for (i, _, _), group in zip(units, loads):
            if (i == order[0]) == array_is_first:
                for copy in group:
                    copy.start()

    load(True)
    norm_loads = [
        pltpu.make_async_copy(ref, in_norm.at[j], norm_sem.at[j])
        for j, ref in enumerate((norm_train, norm_step))
    ]
    for copy in norm_loads:
        copy.start()

    targets = (lax.max(z - 1, 0) * 2 + x, lax.min(z + 1, depth - 1) * 2 + x, z * 2 + 1 - x)
    has = (z >= 1, z <= depth - 2, None)
    first, early_at, early_size = units[0]
    parts = early_send.shape[1]

    def early(way, part):
        size = early_size // parts
        return pltpu.make_async_remote_copy(
            src_ref=wholes[first].at[pl.ds(early_at + part * size, size)],
            dst_ref=in_early.at[way, pl.ds(part * size, size)],
            send_sem=early_send.at[way, part],
            recv_sem=early_recv.at[way, part],
            device_id={"shard": targets[way]},
            device_id_type=MESH,
        )

    def both_ways(way, act):
        if has[way] is None:
            act()
        else:
            pl.when(has[way])(act)

    def send_early(part):
        for way in range(3):
            both_ways(way, lambda way=way: early(way, part).start())

    def block_sums(u, total):
        i, at, size = units[u]
        stage, whole = stages[i], wholes[i]
        group = loop_rows(size, whole.shape[1])

        def update(r, total):
            for j in range(group // 8):
                here = pl.ds(pl.multiple_of(at + r * group + j * 8, 8), 8)
                new = stage[0, here] - learn_rate * (hold_rate * stage[1, here] + stage[2, here])
                whole[here, :] = new
                total = total + jnp.abs(new)
            return total

        return lax.fori_loop(0, size // group, update, total)

    sum_copies = {}
    wid_copies = []
    part = 0
    for i in order:
        mine = [u for u in range(count) if units[u][0] == i]
        total = jnp.zeros((8, wholes[i].shape[1]), jnp.float32)
        for u in mine:
            for copy in loads[u]:
                copy.wait()
        if i == first:
            load(False)
        for u in mine:
            total = block_sums(u, total)
            if i != first and u == mine[len(mine) // 2] and u != mine[0] and part < parts:
                send_early(part)
                part += 1
        sums[i][me] = jnp.sum(total, axis=0, keepdims=True)
        if i == first:
            pl.semaphore_wait(barrier, n - 1 + width - 1)
        sum_copies[i] = []
        for k in range(1, n):
            copy = pltpu.make_async_remote_copy(
                src_ref=sums[i].at[me],
                dst_ref=sums[i].at[me],
                send_sem=sum_send.at[i, k - 1],
                recv_sem=sum_recv.at[i, k - 1],
                device_id={"shard": lax.rem(me + k, n)},
                device_id_type=MESH,
            )
            copy.start()
            sum_copies[i].append(copy)
        if part < parts:
            send_early(part)
            part += 1
        if i == first:
            for copy in norm_loads:
                copy.wait()
            norm_out[me, me_w] = in_norm[0] + in_norm[1]
            for k in range(1, width):
                copy = pltpu.make_async_remote_copy(
                    src_ref=norm_out.at[me, me_w],
                    dst_ref=norm_out.at[me, me_w],
                    send_sem=wid_send.at[k - 1],
                    recv_sem=wid_recv.at[k - 1],
                    device_id={"width": lax.rem(me_w + k, width)},
                    device_id_type=MESH,
                )
                copy.start()
                wid_copies.append(copy)
    for late in range(part, parts):
        send_early(late)

    def piece(owner, u, way, slot):
        i, at, size = units[u]
        where = pl.ds(pl.multiple_of(owner * rows + at, TILE), size)
        return pltpu.make_async_remote_copy(
            src_ref=outs[i].at[where],
            dst_ref=outs[i].at[where],
            send_sem=link_send.at[way, slot, u],
            recv_sem=link_recv.at[way, slot, u],
            device_id={"shard": targets[way]},
            device_id_type=MESH,
        )

    def crosses(source, u):
        low = (z >= 1) & (z < depth // 2) & (source == z - 1)
        high = (z >= depth // 2) & (z <= depth - 2) & (source == z + 1)
        no = low | high
        if u >= half:
            no = no | ((z == 0) & (source == depth - 1)) | ((z == depth - 1) & (source == 0))
        return jnp.logical_not(no)

    def send(owner_z, column, u, way, slot):
        piece(owner_z * 2 + column, u, way, slot).start()

    def narrow(source, source_at, owner, u, factor):
        i, at, size = units[u]
        out = outs[i]
        group = loop_rows(size, out.shape[1])
        scale = jnp.broadcast_to(factor, (group, out.shape[1]))

        def body(r, carry):
            here = pl.ds(pl.multiple_of(source_at + r * group, TILE), group)
            there = pl.ds(pl.multiple_of(owner * rows + at + r * group, TILE), group)
            out[there, :] = (source[here, :] * scale).astype(jnp.bfloat16)
            return carry

        lax.fori_loop(0, size // group, body, 0)

    def early_arrived(way, owner):
        for part in range(parts):
            early(way, part).wait_recv()
        narrow(in_early.at[way], 0, owner, 0, first_factor)

    for i in order:
        for copy in sum_copies[i]:
            copy.wait_recv()
        total = sums[i][0]
        for k in range(1, n):
            total = total + sums[i][k]
        col = total / (rows * n)
        cols[i][...] = col
        factor = 1.0 / col
        if i == first:
            first_factor = factor
        for u in range(count):
            owner, at, size = units[u]
            if owner != i:
                continue
            if u > 0:
                narrow(wholes[i], at, me, u, factor)
                for way in range(3):
                    both_ways(way, lambda u=u, way=way: send(z, x, u, way, 0))
        if i == first:
            narrow(wholes[i], early_at, me, 0, factor)

    for copy in wid_copies:
        copy.wait_recv()
    nrm_copies = []
    for k in range(1, n):
        copy = pltpu.make_async_remote_copy(
            src_ref=norm_out.at[me],
            dst_ref=norm_out.at[me],
            send_sem=nrm_send.at[k - 1],
            recv_sem=nrm_recv.at[k - 1],
            device_id={"shard": lax.rem(me + k, n)},
            device_id_type=MESH,
        )
        copy.start()
        nrm_copies.append(copy)

    last = depth - 1
    low_end, high_end = z <= depth // 2 - 2, z >= depth // 2 + 1

    def arrived(u, way, t, owner):
        if u == 0 and isinstance(t, int) and t == 1:
            early_arrived(way, owner)
        else:
            piece(me, u, way, t - 1).wait_recv()

    def step(t, carry):
        for u in range(count):

            @pl.when(z + t <= last)
            def _(u=u):
                arrived(u, DOWN, t, (z + t) * 2 + x)

                @pl.when(z >= 1)
                def _():
                    send(z + t, x, u, DOWN, t)

                @pl.when(crosses(z + t, u))
                def _():
                    send(z + t, x, u, CROSS, t)

            @pl.when(z - t >= 0)
            def _(u=u):
                arrived(u, UP, t, (z - t) * 2 + x)

                @pl.when(z <= depth - 2)
                def _():
                    send(z - t, x, u, UP, t)

                @pl.when(crosses(z - t, u))
                def _():
                    send(z - t, x, u, CROSS, depth - t)

            if isinstance(t, int):
                if u == 0:
                    early_arrived(CROSS, z * 2 + 1 - x)

                @pl.when(low_end | high_end)
                def _(u=u):
                    if u > 0:
                        piece(me, u, CROSS, 0).wait_recv()

                    @pl.when(low_end)
                    def _():
                        send(z, 1 - x, u, UP, last)

                    @pl.when(high_end)
                    def _():
                        send(z, 1 - x, u, DOWN, last)

            if u >= half:

                @pl.when((t == last) & (z == 1))
                def _(u=u):
                    piece(me, u, CROSS, depth - 2).wait_recv()
                    send(last, 1 - x, u, DOWN, last)

                @pl.when((t == last) & (z == depth - 2))
                def _(u=u):
                    piece(me, u, CROSS, 2).wait_recv()
                    send(0, 1 - x, u, UP, last)

        return carry

    step(1, 0)
    lax.fori_loop(2, depth, step, 0)

    for u in range(1, count):
        seen = low_end | high_end

        @pl.when(jnp.logical_not(seen))
        def _(u=u):
            piece(me, u, CROSS, 0).wait_recv()

    def remaining(t, carry):
        source = lax.rem(z + t, depth)
        for u in range(count):
            owed = crosses(source, u)
            if u >= half:
                seen = ((z == 1) & (source == last)) | ((z == depth - 2) & (source == 0))
                owed = owed & jnp.logical_not(seen)

            @pl.when(owed)
            def _(u=u):
                piece(me, u, CROSS, t).wait_recv()

        return carry

    lax.fori_loop(1, depth, remaining, 0)
    for u in range(count):
        from_above = (z >= depth // 2) & (z <= depth - 2)
        from_below = (z >= 1) & (z < depth // 2)
        if u >= half:
            from_above = from_above | (z == 0)
            from_below = from_below | (z == last)

        @pl.when(from_above)
        def _(u=u):
            piece(me, u, DOWN, last).wait_recv()

        @pl.when(from_below)
        def _(u=u):
            piece(me, u, UP, last).wait_recv()

    for copy in nrm_copies:
        copy.wait_recv()
    for i in order:
        for copy in sum_copies[i]:
            copy.wait_send()
    for copy in wid_copies + nrm_copies:
        copy.wait_send()

    def sent(t, carry):
        source = lax.rem(z + t, depth)
        for u in range(count):
            begun = (u > 0) | (t > 0)

            @pl.when(begun & (z >= 1) & (z + t <= last))
            def _(u=u):
                piece(me, u, DOWN, t).wait_send()

            @pl.when(begun & (z <= depth - 2) & (z - t >= 0))
            def _(u=u):
                piece(me, u, UP, t).wait_send()

            @pl.when(begun & crosses(source, u))
            def _(u=u):
                piece(me, u, CROSS, t).wait_send()

        return carry

    lax.fori_loop(0, depth, sent, 0)
    for part in range(parts):
        for way in range(3):
            both_ways(way, lambda way=way, part=part: early(way, part).wait_send())
    for u in range(count):
        to_above, to_below = low_end, high_end
        if u >= half:
            to_above = to_above | (z == depth - 2)
            to_below = to_below | (z == 1)

        @pl.when(to_above)
        def _(u=u):
            piece(me, u, UP, last).wait_send()

        @pl.when(to_below)
        def _(u=u):
            piece(me, u, DOWN, last).wait_send()


def write_kernel(parts, *refs):
    moved = (len(refs) - 4) // 2
    ins, norm_in, results, norm_out = refs[:moved], refs[moved], refs[moved + 1 : -3], refs[-3]
    norm, sems = refs[-2:]
    norm[...] = norm_in[...].astype(jnp.bfloat16)
    copies = [pltpu.make_async_copy(norm, norm_out, sems.at[0])]
    copies[0].start()
    for i in reversed(range(moved)):
        ref, result = ins[i], results[i]
        pieces = parts[i]
        rows = ref.shape[0] // pieces
        for j in range(pieces):
            where = pl.ds(j * rows, rows)
            copy = pltpu.make_async_copy(ref.at[where], result.at[where], sems.at[len(copies)])
            copy.start()
            copies.append(copy)
    for copy in copies:
        copy.wait()


def local(
    n,
    width,
    w_query,
    first_query,
    second_query,
    w_key,
    first_key,
    second_key,
    w_value,
    first_value,
    second_value,
    norm_train,
    norm_step,
):
    groups = ((w_query, first_query, second_query), (w_key, first_key, second_key), (w_value, first_value, second_value))
    rows = w_query.shape[0]
    extents = [each[0].shape[1] for each in groups]
    units = plan_units(rows, extents)
    early_parts = max(1, min(4, units[0][2] // TILE))
    piece = norm_train.shape[0]
    depth = n // 2
    dma = pltpu.SemaphoreType.DMA
    vmem = pl.BlockSpec(memory_space=pltpu.VMEM)
    hbm = pl.BlockSpec(memory_space=pltpu.HBM)
    shapes = [jax.ShapeDtypeStruct((rows * n, e), jnp.bfloat16) for e in extents]
    shapes += [jax.ShapeDtypeStruct((rows, e), jnp.float32) for e in extents]
    shapes += [jax.ShapeDtypeStruct((1, e), jnp.float32) for e in extents]
    gathered = pl.pallas_call(
        functools.partial(gather_kernel, n, width, units),
        out_shape=shapes + [jax.ShapeDtypeStruct((n, width, 1, piece), jnp.float32)],
        in_specs=[hbm] * 11,
        out_specs=[vmem] * 10,
        scratch_shapes=[pltpu.VMEM((3, rows, e), jnp.float32) for e in extents]
        + [pltpu.VMEM((n, 1, e), jnp.float32) for e in extents]
        + [
            pltpu.VMEM((2, 1, piece), jnp.float32),
            dma((2,)),
            pltpu.VMEM((3, units[0][2], extents[units[0][0]]), jnp.float32),
            dma((3, early_parts)),
            dma((3, early_parts)),
            dma((len(units), 3)),
            dma((3, n - 1)),
            dma((3, n - 1)),
            dma((width - 1,)),
            dma((width - 1,)),
            dma((n - 1,)),
            dma((n - 1,)),
            dma((3, depth, len(units))),
            dma((3, depth, len(units))),
        ],
        compiler_params=pltpu.CompilerParams(
            collective_id=0, has_side_effects=True, vmem_limit_bytes=16 * 1024 * 1024
        ),
    )(
        *[pltpu.with_memory_space_constraint(each, pltpu.HBM) for group in groups for each in group],
        pltpu.with_memory_space_constraint(norm_train.reshape(1, -1), pltpu.HBM),
        pltpu.with_memory_space_constraint(norm_step.reshape(1, -1), pltpu.HBM),
    )
    moved, gain = gathered[:-1], gathered[-1].reshape(-1, 128)
    parts = [max(1, each.size * each.dtype.itemsize // (1 << 20)) for each in moved]
    written = pl.pallas_call(
        functools.partial(write_kernel, parts),
        out_shape=shapes + [jax.ShapeDtypeStruct(gain.shape, jnp.bfloat16)],
        in_specs=[vmem] * 10,
        out_specs=[hbm] * 10,
        scratch_shapes=[pltpu.VMEM(gain.shape, jnp.bfloat16), dma((sum(parts) + 1,))],
        compiler_params=pltpu.CompilerParams(vmem_limit_bytes=16 * 1024 * 1024),
    )(*moved, gain)
    serving, whole, column = written[:3], written[3:6], written[6:9]
    return (*serving, *[each.reshape(-1) for each in column], written[9].reshape(-1), *whole)


def solution(mesh):
    split = P("shard", "width")
    both = P(("shard", "width"))
    n, width = mesh.shape["shard"], mesh.shape["width"]
    return jax.shard_map(
        functools.partial(local, n, width),
        mesh=mesh,
        in_specs=(split,) * 9 + (both, both),
        out_specs=(P(None, "width"),) * 3 + (P("width"),) * 3 + (P(),) + (split,) * 3,
        check_vma=False,
    )
```

```python
import functools
import math

import jax
import jax.numpy as jnp
from jax import lax
from jax.experimental import pallas as pl
from jax.experimental.pallas import tpu as pltpu
from jax.sharding import PartitionSpec as P

learn_rate = 0.2
hold_rate = 0.8
MESH = pl.DeviceIdType.MESH
TILE = 16
DOWN, UP, CROSS = 0, 1, 2


def plan_units(rows, extents):
    least = min(extents)
    units = []
    for i in sorted(range(len(extents)), key=lambda i: extents[i]):
        count = max(1, min(extents[i] // least, rows // TILE))
        size = rows // count
        units += [(i, j * size, size) for j in range(count)]
    return units


def half_of(units, extents):
    sizes = [extents[i] * size for i, _, size in units]
    return min(range(1, len(units)), key=lambda u: abs(2 * sum(sizes[:u]) - sum(sizes)))


def loop_rows(size, extent):
    return math.gcd(size, max(TILE, 16 * 1024 // extent))


def gather_kernel(
    n,
    width,
    units,
    w_q,
    first_q,
    second_q,
    w_k,
    first_k,
    second_k,
    w_v,
    first_v,
    second_v,
    norm_train,
    norm_step,
    out_q,
    out_k,
    out_v,
    whole_q,
    whole_k,
    whole_v,
    col_q,
    col_k,
    col_v,
    norm_out,
    in_q,
    in_k,
    in_v,
    sums_q,
    sums_k,
    sums_v,
    in_norm,
    norm_sem,
    load_sem,
    sum_send,
    sum_recv,
    wid_send,
    wid_recv,
    nrm_send,
    nrm_recv,
    link_send,
    link_recv,
):
    me = lax.axis_index("shard")
    me_w = lax.axis_index("width")
    depth = n // 2
    z, x = lax.div(me, 2), lax.rem(me, 2)
    count = len(units)
    outs, wholes, cols = (out_q, out_k, out_v), (whole_q, whole_k, whole_v), (col_q, col_k, col_v)
    stages, sums = (in_q, in_k, in_v), (sums_q, sums_k, sums_v)
    sources = ((w_q, first_q, second_q), (w_k, first_k, second_k), (w_v, first_v, second_v))
    rows = whole_q.shape[0]
    half = half_of(units, [each.shape[1] for each in wholes])
    order = list(dict.fromkeys(unit[0] for unit in units))

    barrier = pltpu.get_barrier_semaphore()
    for k in range(1, n):
        pl.semaphore_signal(
            barrier, inc=1, device_id={"shard": lax.rem(me + k, n)}, device_id_type=MESH
        )
    for k in range(1, width):
        pl.semaphore_signal(
            barrier, inc=1, device_id={"width": lax.rem(me_w + k, width)}, device_id_type=MESH
        )

    loads = []
    for u, (i, at, size) in enumerate(units):
        group = []
        for j in range(3):
            copy = pltpu.make_async_copy(
                sources[i][j].at[pl.ds(at, size)], stages[i].at[j, pl.ds(at, size)], load_sem.at[u]
            )
            group.append(copy)
        loads.append(group)

    def load(array_is_first):
        for (i, _, _), group in zip(units, loads):
            if (i == order[0]) == array_is_first:
                for copy in group:
                    copy.start()

    load(True)
    norm_loads = [
        pltpu.make_async_copy(ref, in_norm.at[j], norm_sem)
        for j, ref in enumerate((norm_train, norm_step))
    ]
    for copy in norm_loads:
        copy.start()

    targets = (lax.max(z - 1, 0) * 2 + x, lax.min(z + 1, depth - 1) * 2 + x, z * 2 + 1 - x)
    has = (z >= 1, z <= depth - 2, None)
    first = units[0][0]

    def both_ways(way, act):
        if has[way] is None:
            act()
        else:
            pl.when(has[way])(act)

    def block_sums(u, total):
        i, at, size = units[u]
        stage, whole = stages[i], wholes[i]
        group = loop_rows(size, whole.shape[1])

        def update(r, total):
            for j in range(group // 8):
                here = pl.ds(pl.multiple_of(at + r * group + j * 8, 8), 8)
                new = stage[0, here] - learn_rate * (hold_rate * stage[1, here] + stage[2, here])
                whole[here, :] = new
                total = total + jnp.abs(new)
            return total

        return lax.fori_loop(0, size // group, update, total)

    for i in order:
        mine = [u for u in range(count) if units[u][0] == i]
        total = jnp.zeros((8, wholes[i].shape[1]), jnp.float32)
        for u in mine:
            _, at, size = units[u]
            whole_load = stages[i].at[:, pl.ds(at, size)]
            pltpu.make_async_copy(whole_load, whole_load, load_sem.at[u]).wait()
            if u == 0:
                load(False)
            total = block_sums(u, total)
        sums[i][me] = jnp.sum(total, axis=0, keepdims=True)
        if i == first:
            pl.semaphore_wait(barrier, n - 1 + width - 1)
        for k in range(1, n):
            copy = pltpu.make_async_remote_copy(
                src_ref=sums[i].at[me],
                dst_ref=sums[i].at[me],
                send_sem=sum_send.at[i],
                recv_sem=sum_recv.at[i],
                device_id={"shard": lax.rem(me + k, n)},
                device_id_type=MESH,
            )
            copy.start()
        if i == first:
            pltpu.make_async_copy(in_norm, in_norm, norm_sem).wait()
            norm_out[me, me_w] = in_norm[0] + in_norm[1]
            for k in range(1, width):
                copy = pltpu.make_async_remote_copy(
                    src_ref=norm_out.at[me, me_w],
                    dst_ref=norm_out.at[me, me_w],
                    send_sem=wid_send,
                    recv_sem=wid_recv,
                    device_id={"width": lax.rem(me_w + k, width)},
                    device_id_type=MESH,
                )
                copy.start()

    def joint(ref, send_sem, recv_sem):
        return pltpu.make_async_remote_copy(
            src_ref=ref,
            dst_ref=ref,
            send_sem=send_sem,
            recv_sem=recv_sem,
            device_id={"shard": targets[CROSS]},
            device_id_type=MESH,
        )

    halves = (range(half), range(half, count))
    widest = max(range(3), key=lambda i: outs[i].shape[1])

    def bundle(g, way, slot):
        words = sum(units[u][2] * outs[units[u][0]].shape[1] for u in halves[g])
        ref = outs[widest].at[pl.ds(0, words // outs[widest].shape[1])]
        return joint(ref, link_send.at[way, slot, g], link_recv.at[way, slot, g])

    def send_unit(owner_z, column, u, way, slot):
        i, at, size = units[u]
        owner = owner_z * 2 + column
        where = pl.ds(pl.multiple_of(owner * rows + at, TILE), size)
        g = int(u >= half)
        pltpu.make_async_remote_copy(
            src_ref=outs[i].at[where],
            dst_ref=outs[i].at[where],
            send_sem=link_send.at[way, slot, g],
            recv_sem=link_recv.at[way, slot, g],
            device_id={"shard": targets[way]},
            device_id_type=MESH,
        ).start()

    def send(owner_z, column, g, way, slot):
        for u in halves[g]:
            send_unit(owner_z, column, u, way, slot)

    def crosses(source, g):
        low = (z >= 1) & (z < depth // 2) & (source == z - 1)
        high = (z >= depth // 2) & (z <= depth - 2) & (source == z + 1)
        no = low | high
        if g == 1:
            no = no | ((z == 0) & (source == depth - 1)) | ((z == depth - 1) & (source == 0))
        return jnp.logical_not(no)

    def narrow(source, source_at, owner, u, factor):
        i, at, size = units[u]
        out = outs[i]
        group = loop_rows(size, out.shape[1])
        scale = jnp.broadcast_to(factor, (group, out.shape[1]))

        def body(r, carry):
            here = pl.ds(pl.multiple_of(source_at + r * group, TILE), group)
            there = pl.ds(pl.multiple_of(owner * rows + at + r * group, TILE), group)
            out[there, :] = (source[here, :] * scale).astype(jnp.bfloat16)
            return carry

        lax.fori_loop(0, size // group, body, 0)

    for i in order:
        joint(sums[i].at[pl.ds(0, n - 1)], sum_send.at[i], sum_recv.at[i]).wait_recv()
        total = sums[i][0]
        for k in range(1, n):
            total = total + sums[i][k]
        col = total / (rows * n)
        cols[i][...] = col
        factor = 1.0 / col
        for u in range(count):
            owner, at, size = units[u]
            if owner != i:
                continue
            narrow(wholes[i], at, me, u, factor)
            for way in range(3):
                both_ways(way, lambda u=u, way=way: send_unit(z, x, u, way, 0))

    joint(norm_out.at[0, pl.ds(0, width - 1)], wid_send, wid_recv).wait_recv()
    for k in range(1, n):
        copy = pltpu.make_async_remote_copy(
            src_ref=norm_out.at[me],
            dst_ref=norm_out.at[me],
            send_sem=nrm_send,
            recv_sem=nrm_recv,
            device_id={"shard": lax.rem(me + k, n)},
            device_id_type=MESH,
        )
        copy.start()

    last = depth - 1
    low_end, high_end = z <= depth // 2 - 2, z >= depth // 2 + 1

    def step(t, carry):
        for g in range(2):

            @pl.when(z + t <= last)
            def _(g=g):
                bundle(g, DOWN, t - 1).wait_recv()

                @pl.when(z >= 1)
                def _():
                    send(z + t, x, g, DOWN, t)

                swap = (z == 1) & (z + t == last)
                across(z + t, g, t, swap)

            @pl.when(z - t >= 0)
            def _(g=g):
                bundle(g, UP, t - 1).wait_recv()

                @pl.when(z <= depth - 2)
                def _():
                    send(z - t, x, g, UP, t)

                swap = (z == depth - 2) & (z == t)
                across(z - t, g, depth - t, swap)

            @pl.when((t == 1) & (low_end | high_end))
            def _(g=g):
                bundle(g, CROSS, 0).wait_recv()

                @pl.when(low_end)
                def _():
                    send(z, 1 - x, g, UP, last)

                @pl.when(high_end)
                def _():
                    send(z, 1 - x, g, DOWN, last)

        @pl.when((t == last) & (z == 1))
        def _():
            bundle(1, CROSS, depth - 2).wait_recv()
            send(last, 1 - x, 1, DOWN, last)

        @pl.when((t == last) & (z == depth - 2))
        def _():
            bundle(1, CROSS, 2).wait_recv()
            send(0, 1 - x, 1, UP, last)

        return carry

    def across(source, g, slot, swap):
        if g == 0:

            @pl.when(crosses(source, 0) & jnp.logical_not(swap))
            def _():
                send(source, x, 0, CROSS, slot)
        else:

            @pl.when(crosses(source, 1))
            def _():
                send(source, x, 1, CROSS, slot)

            @pl.when(crosses(source, 0) & swap)
            def _():
                send(source, x, 0, CROSS, slot)

    lax.fori_loop(1, depth, step, 0)

    joint(norm_out.at[0, pl.ds(0, width - 1)], wid_send, wid_recv).wait_send()
    for i in order:
        joint(sums[i].at[pl.ds(0, n - 1)], sum_send.at[i], sum_recv.at[i]).wait_send()
    joint(norm_out.at[pl.ds(0, n - 1)], nrm_send, nrm_recv).wait()

    def owed(source, g):
        seen = (source == z) & (low_end | high_end)
        if g == 1:
            seen = seen | ((z == 1) & (source == last)) | ((z == depth - 2) & (source == 0))
        return crosses(source, g) & jnp.logical_not(seen)

    def rest(t, carry):
        above, below = z + t, z - t
        for g in range(2):

            @pl.when((above <= last) & (z >= 1))
            def _(g=g):
                bundle(g, DOWN, t).wait_send()

            @pl.when((below >= 0) & (z <= depth - 2))
            def _(g=g):
                bundle(g, UP, t).wait_send()

            for source, slot, there in (
                (above, t, above <= last),
                (below, depth - t, (t > 0) & (below >= 0)),
            ):

                @pl.when(there & crosses(source, g))
                def _(g=g, slot=slot):
                    bundle(g, CROSS, slot).wait_send()

                @pl.when(there & owed(source, g))
                def _(g=g, slot=slot):
                    bundle(g, CROSS, slot).wait_recv()

        return carry

    lax.fori_loop(0, depth, rest, 0)
    for g in range(2):
        to_above, to_below = low_end, high_end
        from_above = (z >= depth // 2) & (z <= depth - 2)
        from_below = (z >= 1) & (z < depth // 2)
        if g == 1:
            to_above, to_below = to_above | (z == depth - 2), to_below | (z == 1)
            from_above, from_below = from_above | (z == 0), from_below | (z == last)

        @pl.when(to_above)
        def _(g=g):
            bundle(g, UP, last).wait_send()

        @pl.when(to_below)
        def _(g=g):
            bundle(g, DOWN, last).wait_send()

        @pl.when(from_above)
        def _(g=g):
            bundle(g, DOWN, last).wait_recv()

        @pl.when(from_below)
        def _(g=g):
            bundle(g, UP, last).wait_recv()


def write_kernel(*refs):
    moved = (len(refs) - 4) // 2
    ins, norm_in, results, norm_out = refs[:moved], refs[moved], refs[moved + 1 : -3], refs[-3]
    norm, sems = refs[-2:]
    copies = [pltpu.make_async_copy(ins[i], results[i], sems.at[i]) for i in range(moved)]
    for copy in copies:
        copy.start()
    norm[...] = norm_in[...].astype(jnp.bfloat16)
    copies.append(pltpu.make_async_copy(norm, norm_out, sems.at[moved]))
    copies[-1].start()
    for copy in copies:
        copy.wait()


def local(
    n,
    width,
    w_query,
    first_query,
    second_query,
    w_key,
    first_key,
    second_key,
    w_value,
    first_value,
    second_value,
    norm_train,
    norm_step,
):
    groups = ((w_query, first_query, second_query), (w_key, first_key, second_key), (w_value, first_value, second_value))
    rows = w_query.shape[0]
    extents = [each[0].shape[1] for each in groups]
    units = plan_units(rows, extents)
    piece = norm_train.shape[0]
    depth = n // 2
    dma = pltpu.SemaphoreType.DMA
    vmem = pl.BlockSpec(memory_space=pltpu.VMEM)
    hbm = pl.BlockSpec(memory_space=pltpu.HBM)
    shapes = [jax.ShapeDtypeStruct((rows * n, e), jnp.bfloat16) for e in extents]
    shapes += [jax.ShapeDtypeStruct((rows, e), jnp.float32) for e in extents]
    shapes += [jax.ShapeDtypeStruct((1, e), jnp.float32) for e in extents]
    gathered = pl.pallas_call(
        functools.partial(gather_kernel, n, width, units),
        out_shape=shapes + [jax.ShapeDtypeStruct((n, width, 1, piece), jnp.float32)],
        in_specs=[hbm] * 11,
        out_specs=[vmem] * 10,
        scratch_shapes=[pltpu.VMEM((3, rows, e), jnp.float32) for e in extents]
        + [pltpu.VMEM((n, 1, e), jnp.float32) for e in extents]
        + [
            pltpu.VMEM((2, 1, piece), jnp.float32),
            dma(()),
            dma((len(units),)),
            dma((3,)),
            dma((3,)),
            dma(()),
            dma(()),
            dma(()),
            dma(()),
            dma((3, depth, 2)),
            dma((3, depth, 2)),
        ],
        compiler_params=pltpu.CompilerParams(
            collective_id=0, has_side_effects=True, vmem_limit_bytes=16 * 1024 * 1024
        ),
    )(
        *[pltpu.with_memory_space_constraint(each, pltpu.HBM) for group in groups for each in group],
        pltpu.with_memory_space_constraint(norm_train.reshape(1, -1), pltpu.HBM),
        pltpu.with_memory_space_constraint(norm_step.reshape(1, -1), pltpu.HBM),
    )
    moved, gain = gathered[:-1], gathered[-1].reshape(-1, 128)
    written = pl.pallas_call(
        write_kernel,
        out_shape=shapes + [jax.ShapeDtypeStruct(gain.shape, jnp.bfloat16)],
        in_specs=[vmem] * 10,
        out_specs=[hbm] * 10,
        scratch_shapes=[pltpu.VMEM(gain.shape, jnp.bfloat16), dma((len(moved) + 1,))],
        compiler_params=pltpu.CompilerParams(vmem_limit_bytes=16 * 1024 * 1024),
    )(*moved, gain)
    serving, whole, column = written[:3], written[3:6], written[6:9]
    return (*serving, *[each.reshape(-1) for each in column], written[9].reshape(-1), *whole)


def solution(mesh):
    split = P("shard", "width")
    both = P(("shard", "width"))
    n, width = mesh.shape["shard"], mesh.shape["width"]
    return jax.shard_map(
        functools.partial(local, n, width),
        mesh=mesh,
        in_specs=(split,) * 9 + (both, both),
        out_specs=(P(None, "width"),) * 3 + (P("width"),) * 3 + (P(),) + (split,) * 3,
        check_vma=False,
    )
```

```python
import functools
import math

import jax
import jax.numpy as jnp
from jax import lax
from jax.experimental import pallas as pl
from jax.experimental.pallas import tpu as pltpu
from jax.sharding import PartitionSpec as P

learn_rate = 0.2
hold_rate = 0.8
MESH = pl.DeviceIdType.MESH
TILE = 16
DOWN, UP, CROSS = 0, 1, 2


def plan_units(rows, extents):
    wide = extents.index(max(extents))
    units = [(i, 0, rows) for i in range(len(extents)) if i != wide]
    count = 8 if rows % (8 * TILE) == 0 else 4
    return units + [(wide, j * (rows // count), rows // count) for j in range(count)]


def plan_stages(units, extents):
    wide = units[-1][0]
    narrow = [u for u, unit in enumerate(units) if unit[0] != wide]
    rest = [u for u, unit in enumerate(units) if unit[0] == wide]
    count = len(rest)
    cuts = (count // 2, 3 * count // 4) if count >= 8 else (count // 2,)

    def split(chosen):
        sizes = [extents[units[u][0]] * units[u][2] for u in chosen]
        at = min(range(1, len(chosen)), key=lambda k: abs(2 * sum(sizes[:k]) - sum(sizes)))
        return chosen[:at], chosen[at:]

    return [(split(narrow + rest[:cut]), split(rest[cut:])) for cut in cuts]


def loop_rows(size, extent):
    return math.gcd(size, max(TILE, 16 * 1024 // extent))


class Ladder:
    def __init__(self, n, units, halves, place, spare, link_send, link_recv):
        self.depth, self.units, self.halves, self.place, self.spare = n // 2, units, halves, place, spare
        self.link_send, self.link_recv = link_send, link_recv
        me = lax.axis_index("shard")
        self.z, self.x = z, x = lax.div(me, 2), lax.rem(me, 2)
        self.last = last = self.depth - 1
        self.targets = (lax.max(z - 1, 0) * 2 + x, lax.min(z + 1, last) * 2 + x, z * 2 + 1 - x)
        self.low_end, self.high_end = z <= self.depth // 2 - 2, z >= self.depth // 2 + 1

    def joint(self, ref, send_sem, recv_sem):
        return pltpu.make_async_remote_copy(
            src_ref=ref,
            dst_ref=ref,
            send_sem=send_sem,
            recv_sem=recv_sem,
            device_id={"shard": self.targets[CROSS]},
            device_id_type=MESH,
        )

    def bundle(self, g, way, slot):
        words = sum(self.units[u][2] * self.place(u, 0)[0].shape[1] for u in self.halves[g])
        ref = self.spare.at[pl.ds(0, words // self.spare.shape[1])]
        return self.joint(ref, self.link_send.at[way, slot, g], self.link_recv.at[way, slot, g])

    def send_unit(self, owner_z, column, u, way, slot):
        ref, at = self.place(u, owner_z * 2 + column)
        where = pl.ds(pl.multiple_of(at, TILE), self.units[u][2])
        g = int(u in self.halves[1])
        pltpu.make_async_remote_copy(
            src_ref=ref.at[where],
            dst_ref=ref.at[where],
            send_sem=self.link_send.at[way, slot, g],
            recv_sem=self.link_recv.at[way, slot, g],
            device_id={"shard": self.targets[way]},
            device_id_type=MESH,
        ).start()

    def send(self, owner_z, column, g, way, slot):
        for u in self.halves[g]:
            self.send_unit(owner_z, column, u, way, slot)

    def send_own(self, u):
        z, x = self.z, self.x

        @pl.when(z >= 1)
        def _():
            self.send_unit(z, x, u, DOWN, 0)

        @pl.when(z <= self.last - 1)
        def _():
            self.send_unit(z, x, u, UP, 0)

        self.send_unit(z, x, u, CROSS, 0)

    def crosses(self, source, g):
        z, depth, last = self.z, self.depth, self.last
        low = (z >= 1) & (z < depth // 2) & (source == z - 1)
        high = (z >= depth // 2) & (z <= depth - 2) & (source == z + 1)
        no = low | high
        if g == 1:
            no = no | ((z == 0) & (source == last)) | ((z == last) & (source == 0))
        return jnp.logical_not(no)

    def across(self, source, g, slot, swap):
        if g == 0:

            @pl.when(self.crosses(source, 0) & jnp.logical_not(swap))
            def _():
                self.send(source, self.x, 0, CROSS, slot)
        else:

            @pl.when(self.crosses(source, 1))
            def _():
                self.send(source, self.x, 1, CROSS, slot)

            @pl.when(self.crosses(source, 0) & swap)
            def _():
                self.send(source, self.x, 0, CROSS, slot)

    def step(self, t, carry):
        z, x, depth, last = self.z, self.x, self.depth, self.last
        for g in range(2):

            @pl.when(z + t <= last)
            def _(g=g):
                self.bundle(g, DOWN, t - 1).wait_recv()

                @pl.when(z >= 1)
                def _():
                    self.send(z + t, x, g, DOWN, t)

                self.across(z + t, g, t, (z == 1) & (z + t == last))

            @pl.when(z - t >= 0)
            def _(g=g):
                self.bundle(g, UP, t - 1).wait_recv()

                @pl.when(z <= depth - 2)
                def _():
                    self.send(z - t, x, g, UP, t)

                self.across(z - t, g, depth - t, (z == depth - 2) & (z == t))

            @pl.when((t == 1) & (self.low_end | self.high_end))
            def _(g=g):
                self.bundle(g, CROSS, 0).wait_recv()

                @pl.when(self.low_end)
                def _():
                    self.send(z, 1 - x, g, UP, last)

                @pl.when(self.high_end)
                def _():
                    self.send(z, 1 - x, g, DOWN, last)

        @pl.when((t == last) & (z == 1))
        def _():
            self.bundle(1, CROSS, depth - 2).wait_recv()
            self.send(last, 1 - x, 1, DOWN, last)

        @pl.when((t == last) & (z == depth - 2))
        def _():
            self.bundle(1, CROSS, 2).wait_recv()
            self.send(0, 1 - x, 1, UP, last)

        return carry

    def run(self):
        lax.fori_loop(1, self.depth, self.step, 0)

    def finish(self):
        z, depth, last = self.z, self.depth, self.last

        def owed(source, g):
            seen = (source == z) & (self.low_end | self.high_end)
            if g == 1:
                seen = seen | ((z == 1) & (source == last)) | ((z == depth - 2) & (source == 0))
            return self.crosses(source, g) & jnp.logical_not(seen)

        def rest(t, carry):
            above, below = z + t, z - t
            for g in range(2):

                @pl.when((above <= last) & (z >= 1))
                def _(g=g):
                    self.bundle(g, DOWN, t).wait_send()

                @pl.when((below >= 0) & (z <= depth - 2))
                def _(g=g):
                    self.bundle(g, UP, t).wait_send()

                for source, slot, there in (
                    (above, t, above <= last),
                    (below, depth - t, (t > 0) & (below >= 0)),
                ):

                    @pl.when(there & self.crosses(source, g))
                    def _(g=g, slot=slot):
                        self.bundle(g, CROSS, slot).wait_send()

                    @pl.when(there & owed(source, g))
                    def _(g=g, slot=slot):
                        self.bundle(g, CROSS, slot).wait_recv()

            return carry

        lax.fori_loop(0, depth, rest, 0)
        for g in range(2):
            to_above, to_below = self.low_end, self.high_end
            from_above = (z >= depth // 2) & (z <= depth - 2)
            from_below = (z >= 1) & (z < depth // 2)
            if g == 1:
                to_above, to_below = to_above | (z == depth - 2), to_below | (z == 1)
                from_above, from_below = from_above | (z == 0), from_below | (z == last)

            @pl.when(to_above)
            def _(g=g):
                self.bundle(g, UP, last).wait_send()

            @pl.when(to_below)
            def _(g=g):
                self.bundle(g, DOWN, last).wait_send()

            @pl.when(from_above)
            def _(g=g):
                self.bundle(g, DOWN, last).wait_recv()

            @pl.when(from_below)
            def _(g=g):
                self.bundle(g, UP, last).wait_recv()


def by_core(count, body):
    if count == 1:
        body(0)
        return
    core = lax.rem(lax.axis_index("width"), 2)
    for c in range(2):
        pl.when(core == c)(functools.partial(body, c))


def scaled(source, source_at, target, target_at, size, factor):
    extent = target.shape[1]
    group = loop_rows(size, extent)
    scale = jnp.broadcast_to(factor, (group, extent))

    def body(r, carry):
        here = pl.ds(pl.multiple_of(source_at + r * group, TILE), group)
        there = pl.ds(pl.multiple_of(target_at + r * group, TILE), group)
        target[there, :] = (source[here, :] * scale).astype(jnp.bfloat16)
        return carry

    lax.fori_loop(0, size // group, body, 0)


def gather_kernel(
    n,
    width,
    units,
    stages,
    w_q,
    first_q,
    second_q,
    w_k,
    first_k,
    second_k,
    w_v,
    first_v,
    second_v,
    norm_train,
    norm_step,
    low,
    out_k,
    out_v,
    mid,
    whole_q,
    whole_k,
    whole_v,
    col_q,
    col_k,
    col_v,
    norm_out,
    in_q,
    in_k,
    in_v,
    sums_q,
    sums_k,
    sums_v,
    in_norm,
    norm_sem,
    load_sem,
    sum_send,
    sum_recv,
    wid_send,
    wid_recv,
    nrm_send,
    nrm_recv,
    link_send,
    link_recv,
):
    me = lax.axis_index("shard")
    me_w = lax.axis_index("width")
    wholes, cols = (whole_q, whole_k, whole_v), (col_q, col_k, col_v)
    staged, sums = (in_q, in_k, in_v), (sums_q, sums_k, sums_v)
    sources = ((w_q, first_q, second_q), (w_k, first_k, second_k), (w_v, first_v, second_v))
    rows = whole_q.shape[0]
    count = len(units)
    order = list(dict.fromkeys(unit[0] for unit in units))

    barrier = pltpu.get_barrier_semaphore()
    for k in range(1, n):
        pl.semaphore_signal(
            barrier, inc=1, device_id={"shard": lax.rem(me + k, n)}, device_id_type=MESH
        )
    for k in range(1, width):
        pl.semaphore_signal(
            barrier, inc=1, device_id={"width": lax.rem(me_w + k, width)}, device_id_type=MESH
        )

    loads = []
    for u, (i, at, size) in enumerate(units):
        group = []
        for j in range(3):
            copy = pltpu.make_async_copy(
                sources[i][j].at[pl.ds(at, size)], staged[i].at[j, pl.ds(at, size)], load_sem.at[u]
            )
            group.append(copy)
        loads.append(group)

    def load(array_is_first):
        for (i, _, _), group in zip(units, loads):
            if (i == order[0]) == array_is_first:
                for copy in group:
                    copy.start()

    load(True)
    norm_loads = [
        pltpu.make_async_copy(ref, in_norm.at[j], norm_sem)
        for j, ref in enumerate((norm_train, norm_step))
    ]
    for copy in norm_loads:
        copy.start()

    first = units[0][0]

    def block_sums(u, total):
        i, at, size = units[u]
        stage, whole = staged[i], wholes[i]
        group = loop_rows(size, whole.shape[1])

        def update(r, total):
            for j in range(group // 8):
                here = pl.ds(pl.multiple_of(at + r * group + j * 8, 8), 8)
                new = stage[0, here] - learn_rate * (hold_rate * stage[1, here] + stage[2, here])
                whole[here, :] = new
                total = total + jnp.abs(new)
            return total

        return lax.fori_loop(0, size // group, update, total)

    for i in order:
        mine = [u for u in range(count) if units[u][0] == i]
        total = jnp.zeros((8, wholes[i].shape[1]), jnp.float32)
        for u in mine:
            _, at, size = units[u]
            whole_load = staged[i].at[:, pl.ds(at, size)]
            pltpu.make_async_copy(whole_load, whole_load, load_sem.at[u]).wait()
            if u == 0:
                load(False)
            total = block_sums(u, total)
        sums[i][me] = jnp.sum(total, axis=0, keepdims=True)
        if i == first:
            pl.semaphore_wait(barrier, n - 1 + width - 1)
        for k in range(1, n):
            copy = pltpu.make_async_remote_copy(
                src_ref=sums[i].at[me],
                dst_ref=sums[i].at[me],
                send_sem=sum_send.at[i],
                recv_sem=sum_recv.at[i],
                device_id={"shard": lax.rem(me + k, n)},
                device_id_type=MESH,
            )
            copy.start()
        if i == first:
            pltpu.make_async_copy(in_norm, in_norm, norm_sem).wait()
            norm_out[me, me_w] = in_norm[0] + in_norm[1]
            for k in range(1, width):
                copy = pltpu.make_async_remote_copy(
                    src_ref=norm_out.at[me, me_w],
                    dst_ref=norm_out.at[me, me_w],
                    send_sem=wid_send,
                    recv_sem=wid_recv,
                    device_id={"width": lax.rem(me_w + k, width)},
                    device_id_type=MESH,
                )
                copy.start()

    def place(u, owner):
        i, at, _ = units[u]
        if i == 1 or i == 2:
            return (out_k, out_v)[i - 1], owner * rows + at
        if at < rows // 2:
            return low, owner * (rows // 2) + at
        return mid, owner * (rows // 4) + at - rows // 2

    def body(c):
        halves = stages[c][0]
        mine = halves[0] + halves[1]
        ladder = Ladder(n, units, halves, place, low, link_send, link_recv)
        for i in order:
            ladder.joint(sums[i].at[pl.ds(0, n - 1)], sum_send.at[i], sum_recv.at[i]).wait_recv()
            total = sums[i][0]
            for k in range(1, n):
                total = total + sums[i][k]
            col = total / (rows * n)
            cols[i][...] = col
            factor = 1.0 / col
            for u in mine:
                owner, at, size = units[u]
                if owner == i:
                    ref, there = place(u, me)
                    scaled(wholes[i], at, ref, there, size, factor)
                    ladder.send_own(u)
        ladder.joint(norm_out.at[0, pl.ds(0, width - 1)], wid_send, wid_recv).wait_recv()
        for k in range(1, n):
            pltpu.make_async_remote_copy(
                src_ref=norm_out.at[me],
                dst_ref=norm_out.at[me],
                send_sem=nrm_send,
                recv_sem=nrm_recv,
                device_id={"shard": lax.rem(me + k, n)},
                device_id_type=MESH,
            ).start()
        ladder.run()
        ladder.joint(norm_out.at[0, pl.ds(0, width - 1)], wid_send, wid_recv).wait_send()
        for i in order:
            ladder.joint(sums[i].at[pl.ds(0, n - 1)], sum_send.at[i], sum_recv.at[i]).wait_send()
        ladder.joint(norm_out.at[pl.ds(0, n - 1)], nrm_send, nrm_recv).wait()
        ladder.finish()

    by_core(len(stages), body)


def write_first_kernel(
    n,
    kinds,
    low,
    out_k,
    out_v,
    mid,
    whole_q,
    whole_k,
    whole_v,
    col_q,
    col_k,
    col_v,
    norm_in,
    to_q,
    to_k,
    to_v,
    to_whole_q,
    to_whole_k,
    to_whole_v,
    to_col_q,
    to_col_k,
    to_col_v,
    to_norm,
    own,
    norm,
    sems,
):
    rows = whole_q.shape[0]
    pairs = (
        (out_k, to_k),
        (out_v, to_v),
        (whole_q, to_whole_q),
        (whole_k, to_whole_k),
        (whole_v, to_whole_v),
        (col_q, to_col_q),
        (col_k, to_col_k),
        (col_v, to_col_v),
    )
    for j, (ref, result) in enumerate(pairs):
        pltpu.make_async_copy(ref, result, sems.at[j]).start()
    spread(n, rows, low, to_q, 0, sems.at[8])

    def more(c):
        if c == 1:
            spread(n, rows, mid, to_q, rows // 2, sems.at[9])

    by_core(kinds, more)
    norm[...] = norm_in[...].astype(jnp.bfloat16)
    pltpu.make_async_copy(norm, to_norm, sems.at[10]).start()
    scaled(whole_q, rows // 2, own, 0, rows // 2, 1.0 / col_q[...])

    def end(c):
        if c == 1:
            pltpu.make_async_copy(mid, mid, sems.at[9]).wait()

    for j, (ref, result) in enumerate(pairs):
        pltpu.make_async_copy(ref, result, sems.at[j]).wait()
    pltpu.make_async_copy(low, low, sems.at[8]).wait()
    by_core(kinds, end)
    pltpu.make_async_copy(norm, to_norm, sems.at[10]).wait()


def spread(n, rows, ref, result, at, sem):
    size = ref.shape[0] // n

    def body(owner, carry):
        here = pl.ds(pl.multiple_of(owner * size, TILE), size)
        there = pl.ds(pl.multiple_of(owner * rows + at, TILE), size)
        pltpu.make_async_copy(ref.at[here], result.at[there], sem).start()
        return carry

    lax.fori_loop(0, n, body, 0)


def gather_rest_kernel(n, units, stages, rows, own, mid, high, link_send, link_recv):
    me = lax.axis_index("shard")
    quarter = rows // 4

    def place(u, owner):
        at = units[u][1]
        if at < rows // 2 + quarter:
            return mid, owner * quarter + at - rows // 2
        return high, owner * quarter + at - rows // 2 - quarter

    barrier = pltpu.get_barrier_semaphore()
    ladder = Ladder(n, units, stages[0][1], place, high, link_send, link_recv)
    has = (ladder.z >= 1, ladder.z <= ladder.last - 1, ladder.z >= 0)
    for way in range(3):

        @pl.when(has[way])
        def _(way=way):
            pl.semaphore_signal(
                barrier, inc=1, device_id={"shard": ladder.targets[way]}, device_id_type=MESH
            )

    group = loop_rows(quarter, own.shape[1])
    for j, ref in enumerate((mid, high)):

        def keep(r, carry, j=j, ref=ref):
            here = pl.ds(pl.multiple_of(j * quarter + r * group, TILE), group)
            there = pl.ds(pl.multiple_of(me * quarter + r * group, TILE), group)
            ref[there, :] = own[here, :]
            return carry

        lax.fori_loop(0, quarter // group, keep, 0)
    peers = 1 + has[DOWN].astype(jnp.int32) + has[UP].astype(jnp.int32)
    pl.semaphore_wait(barrier, peers)

    def body(c):
        halves = stages[c][1]
        ladder = Ladder(n, units, halves, place, high, link_send, link_recv)
        for u in halves[0] + halves[1]:
            ladder.send_own(u)
        ladder.run()
        ladder.finish()

    by_core(len(stages), body)


def write_rest_kernel(n, kinds, rows, partial, mid, high, result, sems):
    del partial
    spread(n, rows, high, result, 3 * rows // 4, sems.at[0])

    def more(c):
        if c == 0:
            spread(n, rows, mid, result, rows // 2, sems.at[1])
            pltpu.make_async_copy(mid, mid, sems.at[1]).wait()

    by_core(kinds, more)
    pltpu.make_async_copy(high, high, sems.at[0]).wait()


def local(
    n,
    width,
    w_query,
    first_query,
    second_query,
    w_key,
    first_key,
    second_key,
    w_value,
    first_value,
    second_value,
    norm_train,
    norm_step,
):
    groups = ((w_query, first_query, second_query), (w_key, first_key, second_key), (w_value, first_value, second_value))
    rows = w_query.shape[0]
    extents = [each[0].shape[1] for each in groups]
    units = plan_units(rows, extents)
    stages = plan_stages(units, extents)
    kinds = len(stages)
    piece = norm_train.shape[0]
    depth = n // 2
    dma = pltpu.SemaphoreType.DMA
    vmem = pl.BlockSpec(memory_space=pltpu.VMEM)
    hbm = pl.BlockSpec(memory_space=pltpu.HBM)
    serving = [jax.ShapeDtypeStruct((rows * n, e), jnp.bfloat16) for e in extents]
    whole = [jax.ShapeDtypeStruct((rows, e), jnp.float32) for e in extents]
    column = [jax.ShapeDtypeStruct((1, e), jnp.float32) for e in extents]
    wide = extents[0]
    half, quarter = (jax.ShapeDtypeStruct((n * rows // k, wide), jnp.bfloat16) for k in (2, 4))
    links = [dma((3, depth, 2)), dma((3, depth, 2))]
    gathered = pl.pallas_call(
        functools.partial(gather_kernel, n, width, units, stages),
        out_shape=[half, serving[1], serving[2], quarter, *whole, *column]
        + [jax.ShapeDtypeStruct((n, width, 1, piece), jnp.float32)],
        in_specs=[hbm] * 11,
        out_specs=[vmem] * 11,
        scratch_shapes=[pltpu.VMEM((3, rows, e), jnp.float32) for e in extents]
        + [pltpu.VMEM((n, 1, e), jnp.float32) for e in extents]
        + [
            pltpu.VMEM((2, 1, piece), jnp.float32),
            dma(()),
            dma((len(units),)),
            dma((3,)),
            dma((3,)),
            dma(()),
            dma(()),
            dma(()),
            dma(()),
            *links,
        ],
        compiler_params=pltpu.CompilerParams(
            collective_id=0, has_side_effects=True, vmem_limit_bytes=16 * 1024 * 1024
        ),
    )(
        *[pltpu.with_memory_space_constraint(each, pltpu.HBM) for group in groups for each in group],
        pltpu.with_memory_space_constraint(norm_train.reshape(1, -1), pltpu.HBM),
        pltpu.with_memory_space_constraint(norm_step.reshape(1, -1), pltpu.HBM),
    )
    gain = gathered[-1].reshape(-1, 128)
    partial, *written, own = pl.pallas_call(
        functools.partial(write_first_kernel, n, kinds),
        out_shape=[*serving, *whole, *column]
        + [jax.ShapeDtypeStruct(gain.shape, jnp.bfloat16)]
        + [jax.ShapeDtypeStruct((rows // 2, wide), jnp.bfloat16)],
        in_specs=[vmem] * 11,
        out_specs=[hbm] * 10 + [vmem],
        scratch_shapes=[pltpu.VMEM(gain.shape, jnp.bfloat16), dma((11,))],
        compiler_params=pltpu.CompilerParams(vmem_limit_bytes=16 * 1024 * 1024),
    )(*gathered[:-1], gain)
    mid, high = pl.pallas_call(
        functools.partial(gather_rest_kernel, n, units, stages, rows),
        out_shape=[quarter, quarter],
        in_specs=[vmem],
        out_specs=[vmem] * 2,
        scratch_shapes=links,
        compiler_params=pltpu.CompilerParams(
            collective_id=1, has_side_effects=True, vmem_limit_bytes=16 * 1024 * 1024
        ),
    )(own)
    serving_query = pl.pallas_call(
        functools.partial(write_rest_kernel, n, kinds, rows),
        out_shape=serving[0],
        in_specs=[hbm, vmem, vmem],
        out_specs=hbm,
        input_output_aliases={0: 0},
        scratch_shapes=[dma((2,))],
        compiler_params=pltpu.CompilerParams(vmem_limit_bytes=16 * 1024 * 1024),
    )(pltpu.with_memory_space_constraint(partial, pltpu.HBM), mid, high)
    serving_key, serving_value, *rest, norm = written
    wholes, columns = rest[:3], rest[3:]
    return (
        serving_query,
        serving_key,
        serving_value,
        *[each.reshape(-1) for each in columns],
        norm.reshape(-1),
        *wholes,
    )


def solution(mesh):
    split = P("shard", "width")
    both = P(("shard", "width"))
    n, width = mesh.shape["shard"], mesh.shape["width"]
    return jax.shard_map(
        functools.partial(local, n, width),
        mesh=mesh,
        in_specs=(split,) * 9 + (both, both),
        out_specs=(P(None, "width"),) * 3 + (P("width"),) * 3 + (P(),) + (split,) * 3,
        check_vma=False,
    )
```

```python
import functools
import math

import jax
import jax.numpy as jnp
from jax import lax
from jax.experimental import pallas as pl
from jax.experimental.pallas import tpu as pltpu
from jax.sharding import PartitionSpec as P

learn_rate = 0.2
hold_rate = 0.8
MESH = pl.DeviceIdType.MESH
TILE = 16
DOWN, UP, CROSS = 0, 1, 2
CUTS = (0.75, 0.5)
LATER = CUTS.index(max(CUTS))


def plan_units(rows, extents):
    wide = extents.index(max(extents))
    units = [(i, 0, rows) for i in range(len(extents)) if i != wide]
    early = max(TILE, rows // 4)
    units[:1] = [(units[0][0], 0, early), (units[0][0], early, rows - early)]
    count = math.gcd(16, rows // TILE)
    return units + [(wide, j * (rows // count), rows // count) for j in range(count)]


def plan_loads(units, rows):
    wide = units[-1][0]
    count = math.gcd(4, rows // TILE)
    others = dict.fromkeys(unit[0] for unit in units if unit[0] != wide)
    return [(i, 0, rows) for i in others] + [(wide, j * (rows // count), rows // count) for j in range(count)]


def plan_stages(units, extents):
    wide = units[-1][0]
    narrow = [u for u, unit in enumerate(units) if unit[0] != wide]
    rest = [u for u, unit in enumerate(units) if unit[0] == wide]
    count = len(rest)
    cuts = tuple(round(count * cut) for cut in CUTS) if count >= 16 else (count // 2,)

    def split(chosen):
        sizes = [extents[units[u][0]] * units[u][2] for u in chosen]
        at = min(range(1, len(chosen)), key=lambda k: abs(2 * sum(sizes[:k]) - sum(sizes)))
        return chosen[:at], chosen[at:]

    size = units[-1][2]
    stages = [(split(narrow + rest[:cut]), split(rest[cut:])) for cut in cuts]
    return stages, min(cuts) * size, max(cuts) * size


def loop_rows(size, extent):
    return math.gcd(size, max(TILE, 16 * 1024 // extent))


class Ladder:
    def __init__(self, n, units, halves, place, spare, link_send, link_recv, early=None):
        self.early = early
        self.depth, self.units, self.halves, self.place, self.spare = n // 2, units, halves, place, spare
        self.link_send, self.link_recv = link_send, link_recv
        me = lax.axis_index("shard")
        self.z, self.x = z, x = lax.div(me, 2), lax.rem(me, 2)
        self.last = last = self.depth - 1
        self.targets = (lax.max(z - 1, 0) * 2 + x, lax.min(z + 1, last) * 2 + x, z * 2 + 1 - x)
        self.low_end, self.high_end = z <= self.depth // 2 - 2, z >= self.depth // 2 + 1

    def joint(self, ref, send_sem, recv_sem):
        return pltpu.make_async_remote_copy(
            src_ref=ref,
            dst_ref=ref,
            send_sem=send_sem,
            recv_sem=recv_sem,
            device_id={"shard": self.targets[CROSS]},
            device_id_type=MESH,
        )

    def bundle(self, g, way, slot):
        there = [u for u in self.halves[g] if not (self.early and u == 0 and isinstance(slot, int) and slot == 0)]
        words = sum(self.units[u][2] * self.place(u, 0)[0].shape[1] for u in there)
        ref = self.spare.at[pl.ds(0, words // self.spare.shape[1])]
        return self.joint(ref, self.link_send.at[way, slot, g], self.link_recv.at[way, slot, g])

    def send_unit(self, owner_z, column, u, way, slot):
        ref, at = self.place(u, owner_z * 2 + column)
        where = pl.ds(pl.multiple_of(at, TILE), self.units[u][2])
        g = int(u in self.halves[1])
        pltpu.make_async_remote_copy(
            src_ref=ref.at[where],
            dst_ref=ref.at[where],
            send_sem=self.link_send.at[way, slot, g],
            recv_sem=self.link_recv.at[way, slot, g],
            device_id={"shard": self.targets[way]},
            device_id_type=MESH,
        ).start()

    def send(self, owner_z, column, g, way, slot):
        for u in self.halves[g]:
            self.send_unit(owner_z, column, u, way, slot)

    def send_own(self, u):
        z, x = self.z, self.x

        @pl.when(z >= 1)
        def _():
            self.send_unit(z, x, u, DOWN, 0)

        @pl.when(z <= self.last - 1)
        def _():
            self.send_unit(z, x, u, UP, 0)

        self.send_unit(z, x, u, CROSS, 0)

    def crosses(self, source, g):
        z, depth, last = self.z, self.depth, self.last
        low = (z >= 1) & (z < depth // 2) & (source == z - 1)
        high = (z >= depth // 2) & (z <= depth - 2) & (source == z + 1)
        no = low | high
        if g == 1:
            no = no | ((z == 0) & (source == last)) | ((z == last) & (source == 0))
        return jnp.logical_not(no)

    def across(self, source, g, slot, swap):
        if g == 0:

            @pl.when(self.crosses(source, 0) & jnp.logical_not(swap))
            def _():
                self.send(source, self.x, 0, CROSS, slot)
        else:

            @pl.when(self.crosses(source, 1))
            def _():
                self.send(source, self.x, 1, CROSS, slot)

            @pl.when(self.crosses(source, 0) & swap)
            def _():
                self.send(source, self.x, 0, CROSS, slot)

    def step(self, t, carry):
        z, x, depth, last = self.z, self.x, self.depth, self.last
        for g in range(2):

            before = self.early if self.early and g == 0 and isinstance(t, int) else lambda way, owner: None

            @pl.when(z + t <= last)
            def _(g=g, before=before):
                before(DOWN, (z + t) * 2 + x)
                self.bundle(g, DOWN, t - 1).wait_recv()

                @pl.when(z >= 1)
                def _():
                    self.send(z + t, x, g, DOWN, t)

                self.across(z + t, g, t, (z == 1) & (z + t == last))

            @pl.when(z - t >= 0)
            def _(g=g, before=before):
                before(UP, (z - t) * 2 + x)
                self.bundle(g, UP, t - 1).wait_recv()

                @pl.when(z <= depth - 2)
                def _():
                    self.send(z - t, x, g, UP, t)

                self.across(z - t, g, depth - t, (z == depth - 2) & (z == t))

            if not isinstance(t, int):
                continue
            before(CROSS, z * 2 + 1 - x)

            @pl.when(self.low_end | self.high_end)
            def _(g=g):
                self.bundle(g, CROSS, 0).wait_recv()

                @pl.when(self.low_end)
                def _():
                    self.send(z, 1 - x, g, UP, last)

                @pl.when(self.high_end)
                def _():
                    self.send(z, 1 - x, g, DOWN, last)

        @pl.when((t == last) & (z == 1))
        def _():
            self.bundle(1, CROSS, depth - 2).wait_recv()
            self.send(last, 1 - x, 1, DOWN, last)

        @pl.when((t == last) & (z == depth - 2))
        def _():
            self.bundle(1, CROSS, 2).wait_recv()
            self.send(0, 1 - x, 1, UP, last)

        return carry

    def run(self):
        self.step(1, 0)
        lax.fori_loop(2, self.depth, self.step, 0)

    def finish(self):
        z, depth, last = self.z, self.depth, self.last

        def owed(source, g):
            seen = (source == z) & (self.low_end | self.high_end)
            if g == 1:
                seen = seen | ((z == 1) & (source == last)) | ((z == depth - 2) & (source == 0))
            return self.crosses(source, g) & jnp.logical_not(seen)

        def rest(t, carry):
            above, below = z + t, z - t
            for g in range(2):

                @pl.when((above <= last) & (z >= 1))
                def _(g=g):
                    self.bundle(g, DOWN, t).wait_send()

                @pl.when((below >= 0) & (z <= depth - 2))
                def _(g=g):
                    self.bundle(g, UP, t).wait_send()

                both = [(above, t, above <= last)]
                if not isinstance(t, int):
                    both.append((below, depth - t, below >= 0))
                for source, slot, there in both:

                    @pl.when(there & self.crosses(source, g))
                    def _(g=g, slot=slot):
                        self.bundle(g, CROSS, slot).wait_send()

                    @pl.when(there & owed(source, g))
                    def _(g=g, slot=slot):
                        self.bundle(g, CROSS, slot).wait_recv()

            return carry

        rest(0, 0)
        lax.fori_loop(1, depth, rest, 0)
        for g in range(2):
            to_above, to_below = self.low_end, self.high_end
            from_above = (z >= depth // 2) & (z <= depth - 2)
            from_below = (z >= 1) & (z < depth // 2)
            if g == 1:
                to_above, to_below = to_above | (z == depth - 2), to_below | (z == 1)
                from_above, from_below = from_above | (z == 0), from_below | (z == last)

            @pl.when(to_above)
            def _(g=g):
                self.bundle(g, UP, last).wait_send()

            @pl.when(to_below)
            def _(g=g):
                self.bundle(g, DOWN, last).wait_send()

            @pl.when(from_above)
            def _(g=g):
                self.bundle(g, DOWN, last).wait_recv()

            @pl.when(from_below)
            def _(g=g):
                self.bundle(g, UP, last).wait_recv()


def by_core(count, body):
    if count == 1:
        body(0)
        return
    core = lax.rem(lax.axis_index("width"), 2)
    for c in range(2):
        pl.when(core == c)(functools.partial(body, c))


def scaled(source, source_at, target, target_at, size, factor):
    extent = target.shape[1]
    group = loop_rows(size, extent)
    scale = jnp.broadcast_to(factor, (group, extent))

    def body(r, carry):
        here = pl.ds(pl.multiple_of(source_at + r * group, TILE), group)
        there = pl.ds(pl.multiple_of(target_at + r * group, TILE), group)
        target[there, :] = (source[here, :] * scale).astype(jnp.bfloat16)
        return carry

    lax.fori_loop(0, size // group, body, 0)


def gather_kernel(
    n,
    width,
    chunks,
    units,
    stages,
    cut,
    w_q,
    first_q,
    second_q,
    w_k,
    first_k,
    second_k,
    w_v,
    first_v,
    second_v,
    norm_train,
    norm_step,
    low,
    out_k,
    out_v,
    mid,
    whole_q,
    whole_k,
    whole_v,
    col_q,
    col_k,
    col_v,
    norm_out,
    in_q,
    in_k,
    in_v,
    sums_q,
    sums_k,
    sums_v,
    in_norm,
    in_early,
    early_send,
    early_recv,
    norm_sem,
    load_sem,
    sum_send,
    sum_recv,
    wid_send,
    wid_recv,
    nrm_send,
    nrm_recv,
    link_send,
    link_recv,
):
    me = lax.axis_index("shard")
    me_w = lax.axis_index("width")
    wholes, cols = (whole_q, whole_k, whole_v), (col_q, col_k, col_v)
    staged, sums = (in_q, in_k, in_v), (sums_q, sums_k, sums_v)
    sources = ((w_q, first_q, second_q), (w_k, first_k, second_k), (w_v, first_v, second_v))
    rows = whole_q.shape[0]
    order = list(dict.fromkeys(unit[0] for unit in units))

    loads = []
    for u, (i, at, size) in enumerate(chunks):
        group = []
        for j in range(3):
            copy = pltpu.make_async_copy(
                sources[i][j].at[pl.ds(at, size)], staged[i].at[j, pl.ds(at, size)], load_sem.at[u]
            )
            group.append(copy)
        loads.append(group)

    def load(array_is_first):
        for (i, _, _), group in zip(chunks, loads):
            if (i == order[0]) == array_is_first:
                for copy in group:
                    copy.start()

    load(True)
    norm_loads = [
        pltpu.make_async_copy(ref, in_norm.at[j], norm_sem)
        for j, ref in enumerate((norm_train, norm_step))
    ]
    for copy in norm_loads:
        copy.start()

    barrier = pltpu.get_barrier_semaphore()
    for k in range(1, n):
        pl.semaphore_signal(
            barrier, inc=1, device_id={"shard": lax.rem(me + k, n)}, device_id_type=MESH
        )
    for k in range(1, width):
        pl.semaphore_signal(
            barrier, inc=1, device_id={"width": lax.rem(me_w + k, width)}, device_id_type=MESH
        )

    first = units[0][0]

    z, x = lax.div(me, 2), lax.rem(me, 2)
    last = n // 2 - 1
    targets = (lax.max(z - 1, 0) * 2 + x, lax.min(z + 1, last) * 2 + x, z * 2 + 1 - x)
    has = (z >= 1, z <= last - 1, z >= 0)

    def early(way):
        return pltpu.make_async_remote_copy(
            src_ref=wholes[first].at[pl.ds(0, units[0][2])],
            dst_ref=in_early.at[way],
            send_sem=early_send.at[way],
            recv_sem=early_recv.at[way],
            device_id={"shard": targets[way]},
            device_id_type=MESH,
        )

    def early_arrived(way, owner):
        early(way).wait_recv()
        ref, there = place(0, owner)
        scaled(in_early.at[way], 0, ref, there, units[0][2], 1.0 / cols[first][...])

    def block_sums(u, total):
        i, at, size = chunks[u]
        stage, whole = staged[i], wholes[i]
        group = loop_rows(size, whole.shape[1])

        def update(r, total):
            for j in range(group // 8):
                here = pl.ds(pl.multiple_of(at + r * group + j * 8, 8), 8)
                new = stage[0, here] - learn_rate * (hold_rate * stage[1, here] + stage[2, here])
                whole[here, :] = new
                total = total + jnp.abs(new)
            return total

        return lax.fori_loop(0, size // group, update, total)

    for i in order:
        mine = [u for u in range(len(chunks)) if chunks[u][0] == i]
        total = jnp.zeros((8, wholes[i].shape[1]), jnp.float32)
        for u in mine:
            _, at, size = chunks[u]
            whole_load = staged[i].at[:, pl.ds(at, size)]
            pltpu.make_async_copy(whole_load, whole_load, load_sem.at[u]).wait()
            if u == 0:
                load(False)
            total = block_sums(u, total)
        sums[i][me] = jnp.sum(total, axis=0, keepdims=True)
        if i == first:
            pl.semaphore_wait(barrier, n - 1 + width - 1)
        for k in range(1, n):
            copy = pltpu.make_async_remote_copy(
                src_ref=sums[i].at[me],
                dst_ref=sums[i].at[me],
                send_sem=sum_send.at[i],
                recv_sem=sum_recv.at[i],
                device_id={"shard": lax.rem(me + k, n)},
                device_id_type=MESH,
            )
            copy.start()
        if i == order[min(1, len(order) - 1)]:
            for way in range(3):
                pl.when(has[way])(lambda way=way: early(way).start())
        if i == first:
            pltpu.make_async_copy(in_norm, in_norm, norm_sem).wait()
            norm_out[me, me_w] = in_norm[0] + in_norm[1]
            for k in range(1, width):
                copy = pltpu.make_async_remote_copy(
                    src_ref=norm_out.at[me, me_w],
                    dst_ref=norm_out.at[me, me_w],
                    send_sem=wid_send,
                    recv_sem=wid_recv,
                    device_id={"width": lax.rem(me_w + k, width)},
                    device_id_type=MESH,
                )
                copy.start()

    def place(u, owner):
        i, at, _ = units[u]
        if i == 1 or i == 2:
            return (out_k, out_v)[i - 1], owner * rows + at
        if at < cut[0]:
            return low, owner * cut[0] + at
        return mid, owner * (cut[1] - cut[0]) + at - cut[0]

    def body(c):
        halves = stages[c][0]
        mine = halves[0] + halves[1]
        ladder = Ladder(n, units, halves, place, out_k, link_send, link_recv, early_arrived)
        for i in order:
            ladder.joint(sums[i].at[pl.ds(0, n - 1)], sum_send.at[i], sum_recv.at[i]).wait_recv()
            total = sums[i][0]
            for k in range(1, n):
                total = total + sums[i][k]
            col = total / (rows * n)
            cols[i][...] = col
            factor = 1.0 / col
            for u in mine:
                owner, at, size = units[u]
                if owner == i:
                    ref, there = place(u, me)
                    if u > 0:
                        scaled(wholes[i], at, ref, there, size, factor)
                        ladder.send_own(u)
            if i == first:
                ref, there = place(0, me)
                scaled(wholes[i], 0, ref, there, units[0][2], factor)
        ladder.joint(norm_out.at[0, pl.ds(0, width - 1)], wid_send, wid_recv).wait_recv()
        for k in range(1, n):
            pltpu.make_async_remote_copy(
                src_ref=norm_out.at[me],
                dst_ref=norm_out.at[me],
                send_sem=nrm_send,
                recv_sem=nrm_recv,
                device_id={"shard": lax.rem(me + k, n)},
                device_id_type=MESH,
            ).start()
        ladder.run()
        ladder.joint(norm_out.at[0, pl.ds(0, width - 1)], wid_send, wid_recv).wait_send()
        for i in order:
            ladder.joint(sums[i].at[pl.ds(0, n - 1)], sum_send.at[i], sum_recv.at[i]).wait_send()
        ladder.joint(norm_out.at[pl.ds(0, n - 1)], nrm_send, nrm_recv).wait()
        for way in range(3):
            pl.when(has[way])(lambda way=way: early(way).wait_send())
        ladder.finish()

    by_core(len(stages), body)


def write_first_kernel(
    n,
    kinds,
    cut,
    low,
    out_k,
    out_v,
    mid,
    whole_q,
    whole_k,
    whole_v,
    col_q,
    col_k,
    col_v,
    norm_in,
    to_q,
    to_k,
    to_v,
    to_whole_q,
    to_whole_k,
    to_whole_v,
    to_col_q,
    to_col_k,
    to_col_v,
    to_norm,
    own,
    norm,
    sems,
):
    rows = whole_q.shape[0]
    pairs = (
        (out_k, to_k),
        (out_v, to_v),
        (whole_q, to_whole_q),
        (whole_k, to_whole_k),
        (whole_v, to_whole_v),
        (col_q, to_col_q),
        (col_k, to_col_k),
        (col_v, to_col_v),
    )
    for j, (ref, result) in enumerate(pairs):
        pltpu.make_async_copy(ref, result, sems.at[j]).start()
    spread(n, rows, low, to_q, 0, sems.at[8])

    def more(c):
        if kinds > 1 and c == LATER:
            spread(n, rows, mid, to_q, cut[0], sems.at[9])

    by_core(kinds, more)
    norm[...] = norm_in[...].astype(jnp.bfloat16)
    pltpu.make_async_copy(norm, to_norm, sems.at[10]).start()
    scaled(whole_q, cut[0], own, 0, rows - cut[0], 1.0 / col_q[...])

    def end(c):
        if kinds > 1 and c == LATER:
            pltpu.make_async_copy(mid, mid, sems.at[9]).wait()

    for j, (ref, result) in enumerate(pairs):
        pltpu.make_async_copy(ref, result, sems.at[j]).wait()
    pltpu.make_async_copy(low, low, sems.at[8]).wait()
    by_core(kinds, end)
    pltpu.make_async_copy(norm, to_norm, sems.at[10]).wait()


def spread(n, rows, ref, result, at, sem):
    size = ref.shape[0] // n

    def body(owner, carry):
        here = pl.ds(pl.multiple_of(owner * size, TILE), size)
        there = pl.ds(pl.multiple_of(owner * rows + at, TILE), size)
        pltpu.make_async_copy(ref.at[here], result.at[there], sem).start()
        return carry

    lax.fori_loop(0, n, body, 0)


def gather_rest_kernel(n, units, stages, cut, rows, own, mid, high, link_send, link_recv):
    me = lax.axis_index("shard")
    start, end = cut

    def place(u, owner):
        at = units[u][1]
        if at < end:
            return mid, owner * (end - start) + at - start
        return high, owner * (rows - end) + at - end

    barrier = pltpu.get_barrier_semaphore()
    ladder = Ladder(n, units, stages[0][1], place, high, link_send, link_recv)
    has = (ladder.z >= 1, ladder.z <= ladder.last - 1, ladder.z >= 0)
    for way in range(3):

        @pl.when(has[way])
        def _(way=way):
            pl.semaphore_signal(
                barrier, inc=1, device_id={"shard": ladder.targets[way]}, device_id_type=MESH
            )

    for ref, at, size in ((mid, 0, end - start), (high, end - start, rows - end)):
        group = math.gcd(loop_rows(size, own.shape[1]), at)

        def keep(r, carry, ref=ref, at=at, size=size, group=group):
            here = pl.ds(pl.multiple_of(at + r * group, TILE), group)
            there = pl.ds(pl.multiple_of(me * size + r * group, TILE), group)
            ref[there, :] = own[here, :]
            return carry

        if size:
            lax.fori_loop(0, size // group, keep, 0)
    peers = 1 + has[DOWN].astype(jnp.int32) + has[UP].astype(jnp.int32)
    pl.semaphore_wait(barrier, peers)

    def body(c):
        halves = stages[c][1]
        ladder = Ladder(n, units, halves, place, high, link_send, link_recv)
        for u in halves[0] + halves[1]:
            ladder.send_own(u)
        ladder.run()
        ladder.finish()

    by_core(len(stages), body)


def write_rest_kernel(n, kinds, cut, rows, partial, mid, high, result, sems):
    del partial
    spread(n, rows, high, result, cut[1], sems.at[0])

    def more(c):
        if kinds > 1 and c != LATER:
            spread(n, rows, mid, result, cut[0], sems.at[1])
            pltpu.make_async_copy(mid, mid, sems.at[1]).wait()

    by_core(kinds, more)
    pltpu.make_async_copy(high, high, sems.at[0]).wait()


def local(
    n,
    width,
    w_query,
    first_query,
    second_query,
    w_key,
    first_key,
    second_key,
    w_value,
    first_value,
    second_value,
    norm_train,
    norm_step,
):
    groups = ((w_query, first_query, second_query), (w_key, first_key, second_key), (w_value, first_value, second_value))
    rows = w_query.shape[0]
    extents = [each[0].shape[1] for each in groups]
    units = plan_units(rows, extents)
    stages, *cut = plan_stages(units, extents)
    chunks = plan_loads(units, rows)
    kinds = len(stages)
    piece = norm_train.shape[0]
    depth = n // 2
    dma = pltpu.SemaphoreType.DMA
    vmem = pl.BlockSpec(memory_space=pltpu.VMEM)
    hbm = pl.BlockSpec(memory_space=pltpu.HBM)
    serving = [jax.ShapeDtypeStruct((rows * n, e), jnp.bfloat16) for e in extents]
    whole = [jax.ShapeDtypeStruct((rows, e), jnp.float32) for e in extents]
    column = [jax.ShapeDtypeStruct((1, e), jnp.float32) for e in extents]
    wide = extents[0]
    low, mid, high = (
        jax.ShapeDtypeStruct((n * max(size, TILE), wide), jnp.bfloat16)
        for size in (cut[0], cut[1] - cut[0], rows - cut[1])
    )
    links = [dma((3, depth, 2)), dma((3, depth, 2))]
    gathered = pl.pallas_call(
        functools.partial(gather_kernel, n, width, chunks, units, stages, cut),
        out_shape=[low, serving[1], serving[2], mid, *whole, *column]
        + [jax.ShapeDtypeStruct((n, width, 1, piece), jnp.float32)],
        in_specs=[hbm] * 11,
        out_specs=[vmem] * 11,
        scratch_shapes=[pltpu.VMEM((3, rows, e), jnp.float32) for e in extents]
        + [pltpu.VMEM((n, 1, e), jnp.float32) for e in extents]
        + [
            pltpu.VMEM((2, 1, piece), jnp.float32),
            pltpu.VMEM((3, units[0][2], extents[units[0][0]]), jnp.float32),
            dma((3,)),
            dma((3,)),
            dma(()),
            dma((len(chunks),)),
            dma((3,)),
            dma((3,)),
            dma(()),
            dma(()),
            dma(()),
            dma(()),
            *links,
        ],
        compiler_params=pltpu.CompilerParams(
            collective_id=0, has_side_effects=True, vmem_limit_bytes=16 * 1024 * 1024
        ),
    )(
        *[pltpu.with_memory_space_constraint(each, pltpu.HBM) for group in groups for each in group],
        pltpu.with_memory_space_constraint(norm_train.reshape(1, -1), pltpu.HBM),
        pltpu.with_memory_space_constraint(norm_step.reshape(1, -1), pltpu.HBM),
    )
    gain = gathered[-1].reshape(-1, 128)
    partial, *written, own = pl.pallas_call(
        functools.partial(write_first_kernel, n, kinds, cut),
        out_shape=[*serving, *whole, *column]
        + [jax.ShapeDtypeStruct(gain.shape, jnp.bfloat16)]
        + [jax.ShapeDtypeStruct((rows - cut[0], wide), jnp.bfloat16)],
        in_specs=[vmem] * 11,
        out_specs=[hbm] * 10 + [vmem],
        scratch_shapes=[pltpu.VMEM(gain.shape, jnp.bfloat16), dma((11,))],
        compiler_params=pltpu.CompilerParams(vmem_limit_bytes=16 * 1024 * 1024),
    )(*gathered[:-1], gain)
    mid, high = pl.pallas_call(
        functools.partial(gather_rest_kernel, n, units, stages, cut, rows),
        out_shape=[mid, high],
        in_specs=[vmem],
        out_specs=[vmem] * 2,
        scratch_shapes=links,
        compiler_params=pltpu.CompilerParams(
            collective_id=1, has_side_effects=True, vmem_limit_bytes=16 * 1024 * 1024
        ),
    )(own)
    serving_query = pl.pallas_call(
        functools.partial(write_rest_kernel, n, kinds, cut, rows),
        out_shape=serving[0],
        in_specs=[hbm, vmem, vmem],
        out_specs=hbm,
        input_output_aliases={0: 0},
        scratch_shapes=[dma((2,))],
        compiler_params=pltpu.CompilerParams(vmem_limit_bytes=16 * 1024 * 1024),
    )(pltpu.with_memory_space_constraint(partial, pltpu.HBM), mid, high)
    serving_key, serving_value, *rest, norm = written
    wholes, columns = rest[:3], rest[3:]
    return (
        serving_query,
        serving_key,
        serving_value,
        *[each.reshape(-1) for each in columns],
        norm.reshape(-1),
        *wholes,
    )


def solution(mesh):
    split = P("shard", "width")
    both = P(("shard", "width"))
    n, width = mesh.shape["shard"], mesh.shape["width"]
    return jax.shard_map(
        functools.partial(local, n, width),
        mesh=mesh,
        in_specs=(split,) * 9 + (both, both),
        out_specs=(P(None, "width"),) * 3 + (P("width"),) * 3 + (P(),) + (split,) * 3,
        check_vma=False,
    )
```

```python
import functools
import math

import jax
import jax.numpy as jnp
from jax import lax
from jax.experimental import pallas as pl
from jax.experimental.pallas import tpu as pltpu
from jax.sharding import PartitionSpec as P

learn_rate = 0.2
hold_rate = 0.8
MESH = pl.DeviceIdType.MESH
TILE = 16
DOWN, UP, CROSS = 0, 1, 2
CUTS = (0.75, 0.5)
LATER = CUTS.index(max(CUTS))


def plan_units(rows, extents):
    wide = extents.index(max(extents))
    units = [(i, 0, rows) for i in range(len(extents)) if i != wide]
    early = max(TILE, rows // 4)
    units[:1] = [(units[0][0], 0, early), (units[0][0], early, rows - early)]
    count = math.gcd(16, rows // TILE)
    return units + [(wide, j * (rows // count), rows // count) for j in range(count)]


def plan_loads(units, rows):
    wide = units[-1][0]
    count = math.gcd(4, rows // TILE)
    others = dict.fromkeys(unit[0] for unit in units if unit[0] != wide)
    return [(i, 0, rows) for i in others] + [(wide, j * (rows // count), rows // count) for j in range(count)]


def plan_stages(units, extents):
    wide = units[-1][0]
    narrow = [u for u, unit in enumerate(units) if unit[0] != wide]
    rest = [u for u, unit in enumerate(units) if unit[0] == wide]
    count = len(rest)
    cuts = tuple(round(count * cut) for cut in CUTS) if count >= 16 else (count // 2,)

    def split(chosen):
        sizes = [extents[units[u][0]] * units[u][2] for u in chosen]
        at = min(range(1, len(chosen)), key=lambda k: abs(2 * sum(sizes[:k]) - sum(sizes)))
        return chosen[:at], chosen[at:]

    size = units[-1][2]
    stages = [(split(narrow + rest[:cut]), split(rest[cut:])) for cut in cuts]
    return stages, min(cuts) * size, max(cuts) * size


def loop_rows(size, extent):
    return math.gcd(size, max(TILE, 16 * 1024 // extent))


class Ladder:
    def __init__(self, n, units, halves, place, spare, link_send, link_recv, early=None):
        self.early = early
        self.depth, self.units, self.halves, self.place, self.spare = n // 2, units, halves, place, spare
        self.link_send, self.link_recv = link_send, link_recv
        me = lax.axis_index("shard")
        self.z, self.x = z, x = lax.div(me, 2), lax.rem(me, 2)
        self.last = last = self.depth - 1
        self.targets = (lax.max(z - 1, 0) * 2 + x, lax.min(z + 1, last) * 2 + x, z * 2 + 1 - x)
        self.low_end, self.high_end = z <= self.depth // 2 - 2, z >= self.depth // 2 + 1

    def joint(self, ref, send_sem, recv_sem):
        return pltpu.make_async_remote_copy(
            src_ref=ref,
            dst_ref=ref,
            send_sem=send_sem,
            recv_sem=recv_sem,
            device_id={"shard": self.targets[CROSS]},
            device_id_type=MESH,
        )

    def bundle(self, g, way, slot):
        there = [u for u in self.halves[g] if not (self.early and u == 0 and isinstance(slot, int) and slot == 0)]
        words = sum(self.units[u][2] * self.place(u, 0)[0].shape[1] for u in there)
        ref = self.spare.at[pl.ds(0, words // self.spare.shape[1])]
        return self.joint(ref, self.link_send.at[way, slot, g], self.link_recv.at[way, slot, g])

    def send_unit(self, owner_z, column, u, way, slot):
        ref, at = self.place(u, owner_z * 2 + column)
        where = pl.ds(pl.multiple_of(at, TILE), self.units[u][2])
        g = int(u in self.halves[1])
        pltpu.make_async_remote_copy(
            src_ref=ref.at[where],
            dst_ref=ref.at[where],
            send_sem=self.link_send.at[way, slot, g],
            recv_sem=self.link_recv.at[way, slot, g],
            device_id={"shard": self.targets[way]},
            device_id_type=MESH,
        ).start()

    def send(self, owner_z, column, g, way, slot):
        for u in self.halves[g]:
            self.send_unit(owner_z, column, u, way, slot)

    def send_own(self, u):
        z, x = self.z, self.x

        @pl.when(z >= 1)
        def _():
            self.send_unit(z, x, u, DOWN, 0)

        @pl.when(z <= self.last - 1)
        def _():
            self.send_unit(z, x, u, UP, 0)

        self.send_unit(z, x, u, CROSS, 0)

    def crosses(self, source, g):
        z, depth, last = self.z, self.depth, self.last
        low = (z >= 1) & (z < depth // 2) & (source == z - 1)
        high = (z >= depth // 2) & (z <= depth - 2) & (source == z + 1)
        no = low | high
        if g == 1:
            no = no | ((z == 0) & (source == last)) | ((z == last) & (source == 0))
        return jnp.logical_not(no)

    def across(self, source, g, slot, swap):
        if g == 0:

            @pl.when(self.crosses(source, 0) & jnp.logical_not(swap))
            def _():
                self.send(source, self.x, 0, CROSS, slot)
        else:

            @pl.when(self.crosses(source, 1))
            def _():
                self.send(source, self.x, 1, CROSS, slot)

            @pl.when(self.crosses(source, 0) & swap)
            def _():
                self.send(source, self.x, 0, CROSS, slot)

    def step(self, t, carry):
        z, x, depth, last = self.z, self.x, self.depth, self.last
        for g in range(2):

            before = self.early if self.early and g == 0 and isinstance(t, int) else lambda way, owner: None

            @pl.when(z + t <= last)
            def _(g=g, before=before):
                before(DOWN, (z + t) * 2 + x)
                self.bundle(g, DOWN, t - 1).wait_recv()

                @pl.when(z >= 1)
                def _():
                    self.send(z + t, x, g, DOWN, t)

                self.across(z + t, g, t, (z == 1) & (z + t == last))

            @pl.when(z - t >= 0)
            def _(g=g, before=before):
                before(UP, (z - t) * 2 + x)
                self.bundle(g, UP, t - 1).wait_recv()

                @pl.when(z <= depth - 2)
                def _():
                    self.send(z - t, x, g, UP, t)

                self.across(z - t, g, depth - t, (z == depth - 2) & (z == t))

            if not isinstance(t, int):
                continue
            before(CROSS, z * 2 + 1 - x)

            @pl.when(self.low_end | self.high_end)
            def _(g=g):
                self.bundle(g, CROSS, 0).wait_recv()

                @pl.when(self.low_end)
                def _():
                    self.send(z, 1 - x, g, UP, last)

                @pl.when(self.high_end)
                def _():
                    self.send(z, 1 - x, g, DOWN, last)

        @pl.when((t == last) & (z == 1))
        def _():
            self.bundle(1, CROSS, depth - 2).wait_recv()
            self.send(last, 1 - x, 1, DOWN, last)

        @pl.when((t == last) & (z == depth - 2))
        def _():
            self.bundle(1, CROSS, 2).wait_recv()
            self.send(0, 1 - x, 1, UP, last)

        return carry

    def run(self):
        self.step(1, 0)
        lax.fori_loop(2, self.depth, self.step, 0)

    def finish(self):
        z, depth, last = self.z, self.depth, self.last

        def owed(source, g):
            seen = (source == z) & (self.low_end | self.high_end)
            if g == 1:
                seen = seen | ((z == 1) & (source == last)) | ((z == depth - 2) & (source == 0))
            return self.crosses(source, g) & jnp.logical_not(seen)

        def rest(t, carry):
            above, below = z + t, z - t
            for g in range(2):

                @pl.when((above <= last) & (z >= 1))
                def _(g=g):
                    self.bundle(g, DOWN, t).wait_send()

                @pl.when((below >= 0) & (z <= depth - 2))
                def _(g=g):
                    self.bundle(g, UP, t).wait_send()

                both = [(above, t, above <= last)]
                if not isinstance(t, int):
                    both.append((below, depth - t, below >= 0))
                for source, slot, there in both:

                    @pl.when(there & self.crosses(source, g))
                    def _(g=g, slot=slot):
                        self.bundle(g, CROSS, slot).wait_send()

                    @pl.when(there & owed(source, g))
                    def _(g=g, slot=slot):
                        self.bundle(g, CROSS, slot).wait_recv()

            return carry

        rest(0, 0)
        lax.fori_loop(1, depth, rest, 0)
        for g in range(2):
            to_above, to_below = self.low_end, self.high_end
            from_above = (z >= depth // 2) & (z <= depth - 2)
            from_below = (z >= 1) & (z < depth // 2)
            if g == 1:
                to_above, to_below = to_above | (z == depth - 2), to_below | (z == 1)
                from_above, from_below = from_above | (z == 0), from_below | (z == last)

            @pl.when(to_above)
            def _(g=g):
                self.bundle(g, UP, last).wait_send()

            @pl.when(to_below)
            def _(g=g):
                self.bundle(g, DOWN, last).wait_send()

            @pl.when(from_above)
            def _(g=g):
                self.bundle(g, DOWN, last).wait_recv()

            @pl.when(from_below)
            def _(g=g):
                self.bundle(g, UP, last).wait_recv()


def by_core(count, body):
    if count == 1:
        body(0)
        return
    core = lax.rem(lax.axis_index("width"), 2)
    for c in range(2):
        pl.when(core == c)(functools.partial(body, c))


def scaled(source, source_at, target, target_at, size, factor):
    extent = target.shape[1]
    group = loop_rows(size, extent)
    scale = jnp.broadcast_to(factor, (group, extent))

    def body(r, carry):
        here = pl.ds(pl.multiple_of(source_at + r * group, TILE), group)
        there = pl.ds(pl.multiple_of(target_at + r * group, TILE), group)
        target[there, :] = (source[here, :] * scale).astype(jnp.bfloat16)
        return carry

    lax.fori_loop(0, size // group, body, 0)


def gather_kernel(
    n,
    width,
    chunks,
    units,
    stages,
    cut,
    w_q,
    first_q,
    second_q,
    w_k,
    first_k,
    second_k,
    w_v,
    first_v,
    second_v,
    norm_train,
    norm_step,
    low,
    out_k,
    out_v,
    mid,
    whole_q,
    whole_k,
    whole_v,
    col_q,
    col_k,
    col_v,
    norm_out,
    in_q,
    in_k,
    in_v,
    sums_q,
    sums_k,
    sums_v,
    in_norm,
    in_early,
    early_recv,
    norm_sem,
    load_sem,
    sum_recv,
    wid_recv,
    nrm_recv,
    link_recv,
):
    me = lax.axis_index("shard")
    me_w = lax.axis_index("width")
    wholes, cols = (whole_q, whole_k, whole_v), (col_q, col_k, col_v)
    staged, sums = (in_q, in_k, in_v), (sums_q, sums_k, sums_v)
    sources = ((w_q, first_q, second_q), (w_k, first_k, second_k), (w_v, first_v, second_v))
    rows = whole_q.shape[0]
    order = list(dict.fromkeys(unit[0] for unit in units))

    barrier = pltpu.get_barrier_semaphore()
    for k in range(1, n):
        pl.semaphore_signal(
            barrier, inc=1, device_id={"shard": lax.rem(me + k, n)}, device_id_type=MESH
        )
    for k in range(1, width):
        pl.semaphore_signal(
            barrier, inc=1, device_id={"width": lax.rem(me_w + k, width)}, device_id_type=MESH
        )

    loads = []
    for u, (i, at, size) in enumerate(chunks):
        group = []
        for j in range(3):
            copy = pltpu.make_async_copy(
                sources[i][j].at[pl.ds(at, size)], staged[i].at[j, pl.ds(at, size)], load_sem.at[u]
            )
            group.append(copy)
        loads.append(group)

    def load(array_is_first):
        for (i, _, _), group in zip(chunks, loads):
            if (i == order[0]) == array_is_first:
                for copy in group:
                    copy.start()

    load(True)
    norm_loads = [
        pltpu.make_async_copy(ref, in_norm.at[j], norm_sem)
        for j, ref in enumerate((norm_train, norm_step))
    ]
    for copy in norm_loads:
        copy.start()

    dma = pltpu.SemaphoreType.DMA

    def main(early_send, sum_send, wid_send, nrm_send, link_send):
        first = units[0][0]

        z, x = lax.div(me, 2), lax.rem(me, 2)
        last = n // 2 - 1
        targets = (lax.max(z - 1, 0) * 2 + x, lax.min(z + 1, last) * 2 + x, z * 2 + 1 - x)
        has = (z >= 1, z <= last - 1, z >= 0)

        def early(way):
            return pltpu.make_async_remote_copy(
                src_ref=wholes[first].at[pl.ds(0, units[0][2])],
                dst_ref=in_early.at[way],
                send_sem=early_send.at[way],
                recv_sem=early_recv.at[way],
                device_id={"shard": targets[way]},
                device_id_type=MESH,
            )

        def early_arrived(way, owner):
            early(way).wait_recv()
            ref, there = place(0, owner)
            scaled(in_early.at[way], 0, ref, there, units[0][2], 1.0 / cols[first][...])

        def block_sums(u, total):
            i, at, size = chunks[u]
            stage, whole = staged[i], wholes[i]
            group = loop_rows(size, whole.shape[1])

            def update(r, total):
                for j in range(group // 8):
                    here = pl.ds(pl.multiple_of(at + r * group + j * 8, 8), 8)
                    new = stage[0, here] - learn_rate * (hold_rate * stage[1, here] + stage[2, here])
                    whole[here, :] = new
                    total = total + jnp.abs(new)
                return total

            return lax.fori_loop(0, size // group, update, total)

        for i in order:
            mine = [u for u in range(len(chunks)) if chunks[u][0] == i]
            total = jnp.zeros((8, wholes[i].shape[1]), jnp.float32)
            for u in mine:
                _, at, size = chunks[u]
                whole_load = staged[i].at[:, pl.ds(at, size)]
                pltpu.make_async_copy(whole_load, whole_load, load_sem.at[u]).wait()
                if u == 0:
                    load(False)
                total = block_sums(u, total)
            sums[i][me] = jnp.sum(total, axis=0, keepdims=True)
            if i == first:
                pl.semaphore_wait(barrier, n - 1 + width - 1)
            for k in range(1, n):
                copy = pltpu.make_async_remote_copy(
                    src_ref=sums[i].at[me],
                    dst_ref=sums[i].at[me],
                    send_sem=sum_send.at[i],
                    recv_sem=sum_recv.at[i],
                    device_id={"shard": lax.rem(me + k, n)},
                    device_id_type=MESH,
                )
                copy.start()
            if i == order[min(1, len(order) - 1)]:
                for way in range(3):
                    pl.when(has[way])(lambda way=way: early(way).start())
            if i == first:
                pltpu.make_async_copy(in_norm, in_norm, norm_sem).wait()
                norm_out[me, me_w] = in_norm[0] + in_norm[1]
                for k in range(1, width):
                    copy = pltpu.make_async_remote_copy(
                        src_ref=norm_out.at[me, me_w],
                        dst_ref=norm_out.at[me, me_w],
                        send_sem=wid_send,
                        recv_sem=wid_recv,
                        device_id={"width": lax.rem(me_w + k, width)},
                        device_id_type=MESH,
                    )
                    copy.start()

        def place(u, owner):
            i, at, _ = units[u]
            if i == 1 or i == 2:
                return (out_k, out_v)[i - 1], owner * rows + at
            if at < cut[0]:
                return low, owner * cut[0] + at
            return mid, owner * (cut[1] - cut[0]) + at - cut[0]

        def body(c):
            halves = stages[c][0]
            mine = halves[0] + halves[1]
            ladder = Ladder(n, units, halves, place, out_k, link_send, link_recv, early_arrived)
            for i in order:
                ladder.joint(sums[i].at[pl.ds(0, n - 1)], sum_send.at[i], sum_recv.at[i]).wait_recv()
                total = sums[i][0]
                for k in range(1, n):
                    total = total + sums[i][k]
                col = total / (rows * n)
                cols[i][...] = col
                factor = 1.0 / col
                for u in mine:
                    owner, at, size = units[u]
                    if owner == i:
                        ref, there = place(u, me)
                        if u > 0:
                            scaled(wholes[i], at, ref, there, size, factor)
                            ladder.send_own(u)
                if i == first:
                    ref, there = place(0, me)
                    scaled(wholes[i], 0, ref, there, units[0][2], factor)
            ladder.joint(norm_out.at[0, pl.ds(0, width - 1)], wid_send, wid_recv).wait_recv()
            for k in range(1, n):
                pltpu.make_async_remote_copy(
                    src_ref=norm_out.at[me],
                    dst_ref=norm_out.at[me],
                    send_sem=nrm_send,
                    recv_sem=nrm_recv,
                    device_id={"shard": lax.rem(me + k, n)},
                    device_id_type=MESH,
                ).start()
            ladder.run()
            ladder.joint(norm_out.at[0, pl.ds(0, width - 1)], wid_send, wid_recv).wait_send()
            for i in order:
                ladder.joint(sums[i].at[pl.ds(0, n - 1)], sum_send.at[i], sum_recv.at[i]).wait_send()
            ladder.joint(norm_out.at[pl.ds(0, n - 1)], nrm_send, nrm_recv).wait()
            for way in range(3):
                pl.when(has[way])(lambda way=way: early(way).wait_send())
            ladder.finish()

        by_core(len(stages), body)

    pl.run_scoped(main, dma((3,)), dma((3,)), dma(()), dma(()), dma((3, n // 2, 2)))


def write_first_kernel(
    n,
    kinds,
    cut,
    low,
    out_k,
    out_v,
    mid,
    whole_q,
    whole_k,
    whole_v,
    col_q,
    col_k,
    col_v,
    norm_in,
    to_q,
    to_k,
    to_v,
    to_whole_q,
    to_whole_k,
    to_whole_v,
    to_col_q,
    to_col_k,
    to_col_v,
    to_norm,
    own,
    norm,
    sems,
):
    rows = whole_q.shape[0]
    pairs = (
        (out_k, to_k),
        (out_v, to_v),
        (whole_q, to_whole_q),
        (whole_k, to_whole_k),
        (whole_v, to_whole_v),
        (col_q, to_col_q),
        (col_k, to_col_k),
        (col_v, to_col_v),
    )
    for j, (ref, result) in enumerate(pairs):
        pltpu.make_async_copy(ref, result, sems.at[j]).start()
    spread(n, rows, low, to_q, 0, sems.at[8])

    def more(c):
        if kinds > 1 and c == LATER:
            spread(n, rows, mid, to_q, cut[0], sems.at[9])

    by_core(kinds, more)
    norm[...] = norm_in[...].astype(jnp.bfloat16)
    pltpu.make_async_copy(norm, to_norm, sems.at[10]).start()
    scaled(whole_q, cut[0], own, 0, rows - cut[0], 1.0 / col_q[...])

    def end(c):
        if kinds > 1 and c == LATER:
            pltpu.make_async_copy(mid, mid, sems.at[9]).wait()

    for j, (ref, result) in enumerate(pairs):
        pltpu.make_async_copy(ref, result, sems.at[j]).wait()
    pltpu.make_async_copy(low, low, sems.at[8]).wait()
    by_core(kinds, end)
    pltpu.make_async_copy(norm, to_norm, sems.at[10]).wait()


def spread(n, rows, ref, result, at, sem):
    size = ref.shape[0] // n

    def body(owner, carry):
        here = pl.ds(pl.multiple_of(owner * size, TILE), size)
        there = pl.ds(pl.multiple_of(owner * rows + at, TILE), size)
        pltpu.make_async_copy(ref.at[here], result.at[there], sem).start()
        return carry

    lax.fori_loop(0, n, body, 0)


def gather_rest_kernel(n, units, stages, cut, rows, own, mid, high, link_recv):
    me = lax.axis_index("shard")
    start, end = cut

    def place(u, owner):
        at = units[u][1]
        if at < end:
            return mid, owner * (end - start) + at - start
        return high, owner * (rows - end) + at - end

    barrier = pltpu.get_barrier_semaphore()
    ladder = Ladder(n, units, stages[0][1], place, high, None, link_recv)
    has = (ladder.z >= 1, ladder.z <= ladder.last - 1, ladder.z >= 0)
    for way in range(3):

        @pl.when(has[way])
        def _(way=way):
            pl.semaphore_signal(
                barrier, inc=1, device_id={"shard": ladder.targets[way]}, device_id_type=MESH
            )

    for ref, at, size in ((mid, 0, end - start), (high, end - start, rows - end)):
        group = math.gcd(loop_rows(size, own.shape[1]), at)

        def keep(r, carry, ref=ref, at=at, size=size, group=group):
            here = pl.ds(pl.multiple_of(at + r * group, TILE), group)
            there = pl.ds(pl.multiple_of(me * size + r * group, TILE), group)
            ref[there, :] = own[here, :]
            return carry

        if size:
            lax.fori_loop(0, size // group, keep, 0)
    peers = 1 + has[DOWN].astype(jnp.int32) + has[UP].astype(jnp.int32)
    pl.semaphore_wait(barrier, peers)

    def body(link_send, c):
        halves = stages[c][1]
        ladder = Ladder(n, units, halves, place, high, link_send, link_recv)
        for u in halves[0] + halves[1]:
            ladder.send_own(u)
        ladder.run()
        ladder.finish()

    def main(link_send):
        by_core(len(stages), functools.partial(body, link_send))

    pl.run_scoped(main, pltpu.SemaphoreType.DMA((3, n // 2, 2)))


def write_rest_kernel(n, kinds, cut, rows, partial, mid, high, result, sems):
    del partial
    spread(n, rows, high, result, cut[1], sems.at[0])

    def more(c):
        if kinds > 1 and c != LATER:
            spread(n, rows, mid, result, cut[0], sems.at[1])
            pltpu.make_async_copy(mid, mid, sems.at[1]).wait()

    by_core(kinds, more)
    pltpu.make_async_copy(high, high, sems.at[0]).wait()


def local(
    n,
    width,
    w_query,
    first_query,
    second_query,
    w_key,
    first_key,
    second_key,
    w_value,
    first_value,
    second_value,
    norm_train,
    norm_step,
):
    groups = ((w_query, first_query, second_query), (w_key, first_key, second_key), (w_value, first_value, second_value))
    rows = w_query.shape[0]
    extents = [each[0].shape[1] for each in groups]
    units = plan_units(rows, extents)
    stages, *cut = plan_stages(units, extents)
    chunks = plan_loads(units, rows)
    kinds = len(stages)
    piece = norm_train.shape[0]
    depth = n // 2
    dma = pltpu.SemaphoreType.DMA
    vmem = pl.BlockSpec(memory_space=pltpu.VMEM)
    hbm = pl.BlockSpec(memory_space=pltpu.HBM)
    serving = [jax.ShapeDtypeStruct((rows * n, e), jnp.bfloat16) for e in extents]
    whole = [jax.ShapeDtypeStruct((rows, e), jnp.float32) for e in extents]
    column = [jax.ShapeDtypeStruct((1, e), jnp.float32) for e in extents]
    wide = extents[0]
    low, mid, high = (
        jax.ShapeDtypeStruct((n * max(size, TILE), wide), jnp.bfloat16)
        for size in (cut[0], cut[1] - cut[0], rows - cut[1])
    )
    gathered = pl.pallas_call(
        functools.partial(gather_kernel, n, width, chunks, units, stages, cut),
        out_shape=[low, serving[1], serving[2], mid, *whole, *column]
        + [jax.ShapeDtypeStruct((n, width, 1, piece), jnp.float32)],
        in_specs=[hbm] * 11,
        out_specs=[vmem] * 11,
        scratch_shapes=[pltpu.VMEM((3, rows, e), jnp.float32) for e in extents]
        + [pltpu.VMEM((n, 1, e), jnp.float32) for e in extents]
        + [
            pltpu.VMEM((2, 1, piece), jnp.float32),
            pltpu.VMEM((3, units[0][2], extents[units[0][0]]), jnp.float32),
            dma((3,)),
            dma(()),
            dma((len(chunks),)),
            dma((3,)),
            dma(()),
            dma(()),
            dma((3, depth, 2)),
        ],
        compiler_params=pltpu.CompilerParams(
            collective_id=0, has_side_effects=True, vmem_limit_bytes=16 * 1024 * 1024
        ),
    )(
        *[pltpu.with_memory_space_constraint(each, pltpu.HBM) for group in groups for each in group],
        pltpu.with_memory_space_constraint(norm_train.reshape(1, -1), pltpu.HBM),
        pltpu.with_memory_space_constraint(norm_step.reshape(1, -1), pltpu.HBM),
    )
    gain = gathered[-1].reshape(-1, 128)
    partial, *written, own = pl.pallas_call(
        functools.partial(write_first_kernel, n, kinds, cut),
        out_shape=[*serving, *whole, *column]
        + [jax.ShapeDtypeStruct(gain.shape, jnp.bfloat16)]
        + [jax.ShapeDtypeStruct((rows - cut[0], wide), jnp.bfloat16)],
        in_specs=[vmem] * 11,
        out_specs=[hbm] * 10 + [vmem],
        scratch_shapes=[pltpu.VMEM(gain.shape, jnp.bfloat16), dma((11,))],
        compiler_params=pltpu.CompilerParams(vmem_limit_bytes=16 * 1024 * 1024),
    )(*gathered[:-1], gain)
    mid, high = pl.pallas_call(
        functools.partial(gather_rest_kernel, n, units, stages, cut, rows),
        out_shape=[mid, high],
        in_specs=[vmem],
        out_specs=[vmem] * 2,
        scratch_shapes=[dma((3, depth, 2))],
        compiler_params=pltpu.CompilerParams(
            collective_id=1, has_side_effects=True, vmem_limit_bytes=16 * 1024 * 1024
        ),
    )(own)
    serving_query = pl.pallas_call(
        functools.partial(write_rest_kernel, n, kinds, cut, rows),
        out_shape=serving[0],
        in_specs=[hbm, vmem, vmem],
        out_specs=hbm,
        input_output_aliases={0: 0},
        scratch_shapes=[dma((2,))],
        compiler_params=pltpu.CompilerParams(vmem_limit_bytes=16 * 1024 * 1024),
    )(pltpu.with_memory_space_constraint(partial, pltpu.HBM), mid, high)
    serving_key, serving_value, *rest, norm = written
    wholes, columns = rest[:3], rest[3:]
    return (
        serving_query,
        serving_key,
        serving_value,
        *[each.reshape(-1) for each in columns],
        norm.reshape(-1),
        *wholes,
    )


def solution(mesh):
    split = P("shard", "width")
    both = P(("shard", "width"))
    n, width = mesh.shape["shard"], mesh.shape["width"]
    return jax.shard_map(
        functools.partial(local, n, width),
        mesh=mesh,
        in_specs=(split,) * 9 + (both, both),
        out_specs=(P(None, "width"),) * 3 + (P("width"),) * 3 + (P(),) + (split,) * 3,
        check_vma=False,
    )
```

```python
import functools
import math

import jax
import jax.numpy as jnp
from jax import lax
from jax.experimental import pallas as pl
from jax.experimental.pallas import tpu as pltpu
from jax.sharding import PartitionSpec as P

learn_rate = 0.2
hold_rate = 0.8
MESH = pl.DeviceIdType.MESH
TILE = 16
DOWN, UP, CROSS = 0, 1, 2
CUTS = (0.75, 0.5)
LATER = CUTS.index(max(CUTS))


def plan_units(rows, extents):
    wide = extents.index(max(extents))
    units = [(i, 0, rows) for i in range(len(extents)) if i != wide]
    early = max(TILE, rows // 4)
    units[:1] = [(units[0][0], 0, early), (units[0][0], early, rows - early)]
    count = math.gcd(16, rows // TILE)
    return units + [(wide, j * (rows // count), rows // count) for j in range(count)]


def plan_loads(units, rows):
    wide = units[-1][0]
    count = math.gcd(4, rows // TILE)
    others = dict.fromkeys(unit[0] for unit in units if unit[0] != wide)
    return [(i, 0, rows) for i in others] + [(wide, j * (rows // count), rows // count) for j in range(count)]


def plan_stages(units, extents):
    wide = units[-1][0]
    narrow = [u for u, unit in enumerate(units) if unit[0] != wide]
    rest = [u for u, unit in enumerate(units) if unit[0] == wide]
    count = len(rest)
    cuts = tuple(round(count * cut) for cut in CUTS) if count >= 16 else (count // 2,)

    def split(chosen):
        sizes = [extents[units[u][0]] * units[u][2] for u in chosen]
        at = min(range(1, len(chosen)), key=lambda k: abs(2 * sum(sizes[:k]) - sum(sizes)))
        return chosen[:at], chosen[at:]

    size = units[-1][2]
    stages = [(split(narrow + rest[:cut]), split(rest[cut:])) for cut in cuts]
    return stages, min(cuts) * size, max(cuts) * size


def loop_rows(size, extent):
    return math.gcd(size, max(TILE, 16 * 1024 // extent))


class Ladder:
    def __init__(self, n, units, halves, place, spare, link_send, link_recv, early=None):
        self.early = early
        self.depth, self.units, self.halves, self.place, self.spare = n // 2, units, halves, place, spare
        self.link_send, self.link_recv = link_send, link_recv
        me = lax.axis_index("shard")
        self.z, self.x = z, x = lax.div(me, 2), lax.rem(me, 2)
        self.last = last = self.depth - 1
        self.targets = (lax.max(z - 1, 0) * 2 + x, lax.min(z + 1, last) * 2 + x, z * 2 + 1 - x)
        ends = (z == 0) | (z == last)
        self.hot_out, self.hot_in = (z == 1, z == last - 1, ends), (z == 0, z == last, ends)
        self.low_end, self.high_end = z <= self.depth // 2 - 2, z >= self.depth // 2 + 1

    def joint(self, ref, send_sem, recv_sem):
        return pltpu.make_async_remote_copy(
            src_ref=ref,
            dst_ref=ref,
            send_sem=send_sem,
            recv_sem=recv_sem,
            device_id={"shard": self.targets[CROSS]},
            device_id_type=MESH,
        )

    def bundle(self, g, way, slot, without=()):
        words = sum(self.units[u][2] * self.place(u, 0)[0].shape[1] for u in self.halves[g] if u not in without)
        ref = self.spare.at[pl.ds(0, words // self.spare.shape[1])]
        return self.joint(ref, self.link_send.at[way, slot, g], self.link_recv.at[way, slot, g])

    def arrive(self, g, way, slot):
        self.complete(g, way, slot, self.hot_in[way], lambda copy: copy.wait_recv())

    def leave(self, g, way, slot):
        self.complete(g, way, slot, self.hot_out[way], lambda copy: copy.wait_send())

    def complete(self, g, way, slot, hot, wait):
        if self.early and g == 0 and isinstance(slot, int) and slot == 0:

            @pl.when(hot)
            def _():
                wait(self.bundle(g, way, slot, (0,)))

            @pl.when(jnp.logical_not(hot))
            def _():
                wait(self.bundle(g, way, slot))
        else:
            wait(self.bundle(g, way, slot))

    def send_unit(self, owner_z, column, u, way, slot):
        ref, at = self.place(u, owner_z * 2 + column)
        where = pl.ds(pl.multiple_of(at, TILE), self.units[u][2])
        g = int(u in self.halves[1])
        pltpu.make_async_remote_copy(
            src_ref=ref.at[where],
            dst_ref=ref.at[where],
            send_sem=self.link_send.at[way, slot, g],
            recv_sem=self.link_recv.at[way, slot, g],
            device_id={"shard": self.targets[way]},
            device_id_type=MESH,
        ).start()

    def send(self, owner_z, column, g, way, slot):
        for u in self.halves[g]:
            self.send_unit(owner_z, column, u, way, slot)

    def send_own(self, u):
        has = (self.z >= 1, self.z <= self.last - 1, self.z >= 0)
        for way in range(3):
            wanted = has[way]
            if self.early and u == 0:
                wanted = wanted & jnp.logical_not(self.hot_out[way])
            pl.when(wanted)(functools.partial(self.send_unit, self.z, self.x, u, way, 0))

    def crosses(self, source, g):
        z, depth, last = self.z, self.depth, self.last
        low = (z >= 1) & (z < depth // 2) & (source == z - 1)
        high = (z >= depth // 2) & (z <= depth - 2) & (source == z + 1)
        no = low | high
        if g == 1:
            no = no | ((z == 0) & (source == last)) | ((z == last) & (source == 0))
        return jnp.logical_not(no)

    def across(self, source, g, slot, swap):
        if g == 0:

            @pl.when(self.crosses(source, 0) & jnp.logical_not(swap))
            def _():
                self.send(source, self.x, 0, CROSS, slot)
        else:

            @pl.when(self.crosses(source, 1))
            def _():
                self.send(source, self.x, 1, CROSS, slot)

            @pl.when(self.crosses(source, 0) & swap)
            def _():
                self.send(source, self.x, 0, CROSS, slot)

    def step(self, t, carry):
        z, x, depth, last = self.z, self.x, self.depth, self.last
        for g in range(2):

            before = self.early if self.early and g == 0 and isinstance(t, int) else lambda way, owner: None

            @pl.when(z + t <= last)
            def _(g=g, before=before):
                pl.when(self.hot_in[DOWN])(functools.partial(before, DOWN, (z + t) * 2 + x))
                self.arrive(g, DOWN, t - 1)

                @pl.when(z >= 1)
                def _():
                    self.send(z + t, x, g, DOWN, t)

                self.across(z + t, g, t, (z == 1) & (z + t == last))

            @pl.when(z - t >= 0)
            def _(g=g, before=before):
                pl.when(self.hot_in[UP])(functools.partial(before, UP, (z - t) * 2 + x))
                self.arrive(g, UP, t - 1)

                @pl.when(z <= depth - 2)
                def _():
                    self.send(z - t, x, g, UP, t)

                self.across(z - t, g, depth - t, (z == depth - 2) & (z == t))

            if not isinstance(t, int):
                continue
            pl.when(self.hot_in[CROSS])(functools.partial(before, CROSS, z * 2 + 1 - x))

            @pl.when(self.low_end | self.high_end)
            def _(g=g):
                self.arrive(g, CROSS, 0)

                @pl.when(self.low_end)
                def _():
                    self.send(z, 1 - x, g, UP, last)

                @pl.when(self.high_end)
                def _():
                    self.send(z, 1 - x, g, DOWN, last)

        @pl.when((t == last) & (z == 1))
        def _():
            self.arrive(1, CROSS, depth - 2)
            self.send(last, 1 - x, 1, DOWN, last)

        @pl.when((t == last) & (z == depth - 2))
        def _():
            self.arrive(1, CROSS, 2)
            self.send(0, 1 - x, 1, UP, last)

        return carry

    def run(self):
        self.step(1, 0)
        lax.fori_loop(2, self.depth, self.step, 0)

    def finish(self):
        z, depth, last = self.z, self.depth, self.last

        def owed(source, g):
            seen = (source == z) & (self.low_end | self.high_end)
            if g == 1:
                seen = seen | ((z == 1) & (source == last)) | ((z == depth - 2) & (source == 0))
            return self.crosses(source, g) & jnp.logical_not(seen)

        def rest(t, carry):
            above, below = z + t, z - t
            for g in range(2):

                @pl.when((above <= last) & (z >= 1))
                def _(g=g):
                    self.leave(g, DOWN, t)

                @pl.when((below >= 0) & (z <= depth - 2))
                def _(g=g):
                    self.leave(g, UP, t)

                both = [(above, t, above <= last)]
                if not isinstance(t, int):
                    both.append((below, depth - t, below >= 0))
                for source, slot, there in both:

                    @pl.when(there & self.crosses(source, g))
                    def _(g=g, slot=slot):
                        self.leave(g, CROSS, slot)

                    @pl.when(there & owed(source, g))
                    def _(g=g, slot=slot):
                        self.arrive(g, CROSS, slot)

            return carry

        rest(0, 0)
        lax.fori_loop(1, depth, rest, 0)
        for g in range(2):
            to_above, to_below = self.low_end, self.high_end
            from_above = (z >= depth // 2) & (z <= depth - 2)
            from_below = (z >= 1) & (z < depth // 2)
            if g == 1:
                to_above, to_below = to_above | (z == depth - 2), to_below | (z == 1)
                from_above, from_below = from_above | (z == 0), from_below | (z == last)

            @pl.when(to_above)
            def _(g=g):
                self.leave(g, UP, last)

            @pl.when(to_below)
            def _(g=g):
                self.leave(g, DOWN, last)

            @pl.when(from_above)
            def _(g=g):
                self.arrive(g, DOWN, last)

            @pl.when(from_below)
            def _(g=g):
                self.arrive(g, UP, last)


def by_core(count, body):
    if count == 1:
        body(0)
        return
    core = lax.rem(lax.axis_index("width"), 2)
    for c in range(2):
        pl.when(core == c)(functools.partial(body, c))


def scaled(source, source_at, target, target_at, size, factor):
    extent = target.shape[1]
    group = loop_rows(size, extent)
    scale = jnp.broadcast_to(factor, (group, extent))

    def body(r, carry):
        here = pl.ds(pl.multiple_of(source_at + r * group, TILE), group)
        there = pl.ds(pl.multiple_of(target_at + r * group, TILE), group)
        target[there, :] = (source[here, :] * scale).astype(jnp.bfloat16)
        return carry

    lax.fori_loop(0, size // group, body, 0)


def gather_kernel(
    n,
    width,
    chunks,
    units,
    stages,
    cut,
    w_q,
    first_q,
    second_q,
    w_k,
    first_k,
    second_k,
    w_v,
    first_v,
    second_v,
    norm_train,
    norm_step,
    low,
    out_k,
    out_v,
    mid,
    whole_q,
    whole_k,
    whole_v,
    col_q,
    col_k,
    col_v,
    norm_out,
    in_q,
    in_k,
    in_v,
    sums_q,
    sums_k,
    sums_v,
    in_norm,
    in_early,
    early_send,
    early_recv,
    norm_sem,
    load_sem,
    sum_send,
    sum_recv,
    wid_send,
    wid_recv,
    nrm_send,
    nrm_recv,
    link_send,
    link_recv,
):
    me = lax.axis_index("shard")
    me_w = lax.axis_index("width")
    wholes, cols = (whole_q, whole_k, whole_v), (col_q, col_k, col_v)
    staged, sums = (in_q, in_k, in_v), (sums_q, sums_k, sums_v)
    sources = ((w_q, first_q, second_q), (w_k, first_k, second_k), (w_v, first_v, second_v))
    rows = whole_q.shape[0]
    order = list(dict.fromkeys(unit[0] for unit in units))

    loads = []
    for u, (i, at, size) in enumerate(chunks):
        group = []
        for j in range(3):
            copy = pltpu.make_async_copy(
                sources[i][j].at[pl.ds(at, size)], staged[i].at[j, pl.ds(at, size)], load_sem.at[u]
            )
            group.append(copy)
        loads.append(group)

    def load(array_is_first):
        for (i, _, _), group in zip(chunks, loads):
            if (i == order[0]) == array_is_first:
                for copy in group:
                    copy.start()

    load(True)
    norm_loads = [
        pltpu.make_async_copy(ref, in_norm.at[j], norm_sem)
        for j, ref in enumerate((norm_train, norm_step))
    ]
    for copy in norm_loads:
        copy.start()

    barrier = pltpu.get_barrier_semaphore()
    for k in range(1, n):
        pl.semaphore_signal(
            barrier, inc=1, device_id={"shard": lax.rem(me + k, n)}, device_id_type=MESH
        )
    for k in range(1, width):
        pl.semaphore_signal(
            barrier, inc=1, device_id={"width": lax.rem(me_w + k, width)}, device_id_type=MESH
        )

    first = units[0][0]

    z, x = lax.div(me, 2), lax.rem(me, 2)
    last = n // 2 - 1
    targets = (lax.max(z - 1, 0) * 2 + x, lax.min(z + 1, last) * 2 + x, z * 2 + 1 - x)
    hot = (z == 1, z == last - 1, (z == 0) | (z == last))

    def early(way):
        return pltpu.make_async_remote_copy(
            src_ref=wholes[first].at[pl.ds(0, units[0][2])],
            dst_ref=in_early.at[way],
            send_sem=early_send.at[way],
            recv_sem=early_recv.at[way],
            device_id={"shard": targets[way]},
            device_id_type=MESH,
        )

    def early_arrived(way, owner):
        early(way).wait_recv()
        ref, there = place(0, owner)
        scaled(in_early.at[way], 0, ref, there, units[0][2], 1.0 / cols[first][...])

    def block_sums(u, total):
        i, at, size = chunks[u]
        stage, whole = staged[i], wholes[i]
        group = loop_rows(size, whole.shape[1])

        def update(r, total):
            for j in range(group // 8):
                here = pl.ds(pl.multiple_of(at + r * group + j * 8, 8), 8)
                new = stage[0, here] - learn_rate * (hold_rate * stage[1, here] + stage[2, here])
                whole[here, :] = new
                total = total + jnp.abs(new)
            return total

        return lax.fori_loop(0, size // group, update, total)

    for i in order:
        mine = [u for u in range(len(chunks)) if chunks[u][0] == i]
        total = jnp.zeros((8, wholes[i].shape[1]), jnp.float32)
        for u in mine:
            _, at, size = chunks[u]
            whole_load = staged[i].at[:, pl.ds(at, size)]
            pltpu.make_async_copy(whole_load, whole_load, load_sem.at[u]).wait()
            if u == 0:
                load(False)
            total = block_sums(u, total)
        sums[i][me] = jnp.sum(total, axis=0, keepdims=True)
        if i == first:
            pl.semaphore_wait(barrier, n - 1 + width - 1)
        for k in range(1, n):
            copy = pltpu.make_async_remote_copy(
                src_ref=sums[i].at[me],
                dst_ref=sums[i].at[me],
                send_sem=sum_send.at[i],
                recv_sem=sum_recv.at[i],
                device_id={"shard": lax.rem(me + k, n)},
                device_id_type=MESH,
            )
            copy.start()
        if i == order[min(1, len(order) - 1)]:
            for way in range(3):
                pl.when(hot[way])(lambda way=way: early(way).start())
        if i == first:
            pltpu.make_async_copy(in_norm, in_norm, norm_sem).wait()
            norm_out[me, me_w] = in_norm[0] + in_norm[1]
            for k in range(1, width):
                copy = pltpu.make_async_remote_copy(
                    src_ref=norm_out.at[me, me_w],
                    dst_ref=norm_out.at[me, me_w],
                    send_sem=wid_send,
                    recv_sem=wid_recv,
                    device_id={"width": lax.rem(me_w + k, width)},
                    device_id_type=MESH,
                )
                copy.start()

    def place(u, owner):
        i, at, _ = units[u]
        if i == 1 or i == 2:
            return (out_k, out_v)[i - 1], owner * rows + at
        if at < cut[0]:
            return low, owner * cut[0] + at
        return mid, owner * (cut[1] - cut[0]) + at - cut[0]

    def body(c):
        halves = stages[c][0]
        mine = halves[0] + halves[1]
        ladder = Ladder(n, units, halves, place, out_k, link_send, link_recv, early_arrived)
        for i in order:
            ladder.joint(sums[i].at[pl.ds(0, n - 1)], sum_send.at[i], sum_recv.at[i]).wait_recv()
            total = sums[i][0]
            for k in range(1, n):
                total = total + sums[i][k]
            col = total / (rows * n)
            cols[i][...] = col
            factor = 1.0 / col
            for u in mine:
                owner, at, size = units[u]
                if owner == i:
                    ref, there = place(u, me)
                    scaled(wholes[i], at, ref, there, size, factor)
                    ladder.send_own(u)
        ladder.joint(norm_out.at[0, pl.ds(0, width - 1)], wid_send, wid_recv).wait_recv()
        for k in range(1, n):
            pltpu.make_async_remote_copy(
                src_ref=norm_out.at[me],
                dst_ref=norm_out.at[me],
                send_sem=nrm_send,
                recv_sem=nrm_recv,
                device_id={"shard": lax.rem(me + k, n)},
                device_id_type=MESH,
            ).start()
        ladder.run()
        ladder.joint(norm_out.at[0, pl.ds(0, width - 1)], wid_send, wid_recv).wait_send()
        for i in order:
            ladder.joint(sums[i].at[pl.ds(0, n - 1)], sum_send.at[i], sum_recv.at[i]).wait_send()
        ladder.joint(norm_out.at[pl.ds(0, n - 1)], nrm_send, nrm_recv).wait()
        for way in range(3):
            pl.when(hot[way])(lambda way=way: early(way).wait_send())
        ladder.finish()

    by_core(len(stages), body)


def write_first_kernel(
    n,
    kinds,
    cut,
    low,
    out_k,
    out_v,
    mid,
    whole_q,
    whole_k,
    whole_v,
    col_q,
    col_k,
    col_v,
    norm_in,
    to_q,
    to_k,
    to_v,
    to_whole_q,
    to_whole_k,
    to_whole_v,
    to_col_q,
    to_col_k,
    to_col_v,
    to_norm,
    own,
    norm,
    sems,
):
    rows = whole_q.shape[0]
    pairs = (
        (out_k, to_k),
        (out_v, to_v),
        (whole_q, to_whole_q),
        (whole_k, to_whole_k),
        (whole_v, to_whole_v),
        (col_q, to_col_q),
        (col_k, to_col_k),
        (col_v, to_col_v),
    )
    for j, (ref, result) in enumerate(pairs):
        pltpu.make_async_copy(ref, result, sems.at[j]).start()
    spread(n, rows, low, to_q, 0, sems.at[8])

    def more(c):
        if kinds > 1 and c == LATER:
            spread(n, rows, mid, to_q, cut[0], sems.at[9])

    by_core(kinds, more)
    norm[...] = norm_in[...].astype(jnp.bfloat16)
    pltpu.make_async_copy(norm, to_norm, sems.at[10]).start()
    scaled(whole_q, cut[0], own, 0, rows - cut[0], 1.0 / col_q[...])

    def end(c):
        if kinds > 1 and c == LATER:
            pltpu.make_async_copy(mid, mid, sems.at[9]).wait()

    for j, (ref, result) in enumerate(pairs):
        pltpu.make_async_copy(ref, result, sems.at[j]).wait()
    pltpu.make_async_copy(low, low, sems.at[8]).wait()
    by_core(kinds, end)
    pltpu.make_async_copy(norm, to_norm, sems.at[10]).wait()


def spread(n, rows, ref, result, at, sem):
    size = ref.shape[0] // n

    def body(owner, carry):
        here = pl.ds(pl.multiple_of(owner * size, TILE), size)
        there = pl.ds(pl.multiple_of(owner * rows + at, TILE), size)
        pltpu.make_async_copy(ref.at[here], result.at[there], sem).start()
        return carry

    lax.fori_loop(0, n, body, 0)


def gather_rest_kernel(n, units, stages, cut, rows, own, mid, high, link_send, link_recv):
    me = lax.axis_index("shard")
    start, end = cut

    def place(u, owner):
        at = units[u][1]
        if at < end:
            return mid, owner * (end - start) + at - start
        return high, owner * (rows - end) + at - end

    barrier = pltpu.get_barrier_semaphore()
    ladder = Ladder(n, units, stages[0][1], place, high, link_send, link_recv)
    has = (ladder.z >= 1, ladder.z <= ladder.last - 1, ladder.z >= 0)
    for way in range(3):

        @pl.when(has[way])
        def _(way=way):
            pl.semaphore_signal(
                barrier, inc=1, device_id={"shard": ladder.targets[way]}, device_id_type=MESH
            )

    for ref, at, size in ((mid, 0, end - start), (high, end - start, rows - end)):
        group = math.gcd(loop_rows(size, own.shape[1]), at)

        def keep(r, carry, ref=ref, at=at, size=size, group=group):
            here = pl.ds(pl.multiple_of(at + r * group, TILE), group)
            there = pl.ds(pl.multiple_of(me * size + r * group, TILE), group)
            ref[there, :] = own[here, :]
            return carry

        if size:
            lax.fori_loop(0, size // group, keep, 0)
    peers = 1 + has[DOWN].astype(jnp.int32) + has[UP].astype(jnp.int32)
    pl.semaphore_wait(barrier, peers)

    def body(c):
        halves = stages[c][1]
        ladder = Ladder(n, units, halves, place, high, link_send, link_recv)
        for u in halves[0] + halves[1]:
            ladder.send_own(u)
        ladder.run()
        ladder.finish()

    by_core(len(stages), body)


def write_rest_kernel(n, kinds, cut, rows, partial, mid, high, result, sems):
    del partial
    spread(n, rows, high, result, cut[1], sems.at[0])

    def more(c):
        if kinds > 1 and c != LATER:
            spread(n, rows, mid, result, cut[0], sems.at[1])
            pltpu.make_async_copy(mid, mid, sems.at[1]).wait()

    by_core(kinds, more)
    pltpu.make_async_copy(high, high, sems.at[0]).wait()


def local(
    n,
    width,
    w_query,
    first_query,
    second_query,
    w_key,
    first_key,
    second_key,
    w_value,
    first_value,
    second_value,
    norm_train,
    norm_step,
):
    groups = ((w_query, first_query, second_query), (w_key, first_key, second_key), (w_value, first_value, second_value))
    rows = w_query.shape[0]
    extents = [each[0].shape[1] for each in groups]
    units = plan_units(rows, extents)
    stages, *cut = plan_stages(units, extents)
    chunks = plan_loads(units, rows)
    kinds = len(stages)
    piece = norm_train.shape[0]
    depth = n // 2
    dma = pltpu.SemaphoreType.DMA
    vmem = pl.BlockSpec(memory_space=pltpu.VMEM)
    hbm = pl.BlockSpec(memory_space=pltpu.HBM)
    serving = [jax.ShapeDtypeStruct((rows * n, e), jnp.bfloat16) for e in extents]
    whole = [jax.ShapeDtypeStruct((rows, e), jnp.float32) for e in extents]
    column = [jax.ShapeDtypeStruct((1, e), jnp.float32) for e in extents]
    wide = extents[0]
    low, mid, high = (
        jax.ShapeDtypeStruct((n * max(size, TILE), wide), jnp.bfloat16)
        for size in (cut[0], cut[1] - cut[0], rows - cut[1])
    )
    links = [dma((3, depth, 2)), dma((3, depth, 2))]
    gathered = pl.pallas_call(
        functools.partial(gather_kernel, n, width, chunks, units, stages, cut),
        out_shape=[low, serving[1], serving[2], mid, *whole, *column]
        + [jax.ShapeDtypeStruct((n, width, 1, piece), jnp.float32)],
        in_specs=[hbm] * 11,
        out_specs=[vmem] * 11,
        scratch_shapes=[pltpu.VMEM((3, rows, e), jnp.float32) for e in extents]
        + [pltpu.VMEM((n, 1, e), jnp.float32) for e in extents]
        + [
            pltpu.VMEM((2, 1, piece), jnp.float32),
            pltpu.VMEM((3, units[0][2], extents[units[0][0]]), jnp.float32),
            dma((3,)),
            dma((3,)),
            dma(()),
            dma((len(chunks),)),
            dma((3,)),
            dma((3,)),
            dma(()),
            dma(()),
            dma(()),
            dma(()),
            *links,
        ],
        compiler_params=pltpu.CompilerParams(
            collective_id=0, has_side_effects=True, vmem_limit_bytes=16 * 1024 * 1024
        ),
    )(
        *[pltpu.with_memory_space_constraint(each, pltpu.HBM) for group in groups for each in group],
        pltpu.with_memory_space_constraint(norm_train.reshape(1, -1), pltpu.HBM),
        pltpu.with_memory_space_constraint(norm_step.reshape(1, -1), pltpu.HBM),
    )
    gain = gathered[-1].reshape(-1, 128)
    partial, *written, own = pl.pallas_call(
        functools.partial(write_first_kernel, n, kinds, cut),
        out_shape=[*serving, *whole, *column]
        + [jax.ShapeDtypeStruct(gain.shape, jnp.bfloat16)]
        + [jax.ShapeDtypeStruct((rows - cut[0], wide), jnp.bfloat16)],
        in_specs=[vmem] * 11,
        out_specs=[hbm] * 10 + [vmem],
        scratch_shapes=[pltpu.VMEM(gain.shape, jnp.bfloat16), dma((11,))],
        compiler_params=pltpu.CompilerParams(vmem_limit_bytes=16 * 1024 * 1024),
    )(*gathered[:-1], gain)
    mid, high = pl.pallas_call(
        functools.partial(gather_rest_kernel, n, units, stages, cut, rows),
        out_shape=[mid, high],
        in_specs=[vmem],
        out_specs=[vmem] * 2,
        scratch_shapes=links,
        compiler_params=pltpu.CompilerParams(
            collective_id=1, has_side_effects=True, vmem_limit_bytes=16 * 1024 * 1024
        ),
    )(own)
    serving_query = pl.pallas_call(
        functools.partial(write_rest_kernel, n, kinds, cut, rows),
        out_shape=serving[0],
        in_specs=[hbm, vmem, vmem],
        out_specs=hbm,
        input_output_aliases={0: 0},
        scratch_shapes=[dma((2,))],
        compiler_params=pltpu.CompilerParams(vmem_limit_bytes=16 * 1024 * 1024),
    )(pltpu.with_memory_space_constraint(partial, pltpu.HBM), mid, high)
    serving_key, serving_value, *rest, norm = written
    wholes, columns = rest[:3], rest[3:]
    return (
        serving_query,
        serving_key,
        serving_value,
        *[each.reshape(-1) for each in columns],
        norm.reshape(-1),
        *wholes,
    )


def solution(mesh):
    split = P("shard", "width")
    both = P(("shard", "width"))
    n, width = mesh.shape["shard"], mesh.shape["width"]
    return jax.shard_map(
        functools.partial(local, n, width),
        mesh=mesh,
        in_specs=(split,) * 9 + (both, both),
        out_specs=(P(None, "width"),) * 3 + (P("width"),) * 3 + (P(),) + (split,) * 3,
        check_vma=False,
    )
```
